32 devices in a mesh: row: 4 (over x, core), col: 8 (over z, y).
Axes of the slice: x: 2, y: 2, z: 4, core: 2. Of those that a mesh axis runs over, the one named last changes fastest.
Arguments:
- weight: bfloat16 [16384, 16384], P('row', 'col'), may hold values from -0.046875 to 0.046875
- momentum: float32 [16384, 16384], P('row', 'col'), may hold values from -36 to 36
- right_factor: float32 [16384, 512], P(('col', 'row')), may hold values from -0.046875 to 0.046875
- output_grads: bfloat16 [1024, 16384], P('col', 'row'), may hold values from -0.1875 to 0.1875
- activations: bfloat16 [1024, 16384], P('row', 'col'), may hold values from -6 to 6
Outputs:
- new_weight: bfloat16 [16384, 16384], P('row', 'col')
- new_momentum: float32 [16384, 16384], P('row', 'col')
- new_factor: float32 [16384, 512], P(('col', 'row'))
The draws below stay inside these ranges and needn't reach their ends.
All inputs are finite; a program needn't handle non-finite values.
Results may differ from the reference program's by a relative error of at most 0.0004.
Values may be sent and summed in bfloat16 or wider, within the bound.
No kernel may reach another device: no remote copies, remote signals or barrier semaphores. Data moves between devices by JAX's collectives and lax.ppermute only.
A program may use at most 192 MiB of HBM per device.

```python
import math
import jax
import jax.numpy as jnp
from jax import lax

D_OUT = 16384
D_IN = 16384
RANK = 512
TOK = 1024
BLOCK_ROWS = 512


def scaled_field(key, rows, cols):
    first = jax.random.fold_in(key, 0)
    return jax.random.truncated_normal(first, -6.0, 6.0, (rows, cols), jnp.float32)


def draw_momentum(key, part):
    first, second = jax.random.split(jax.random.fold_in(key, 11))
    blocks = D_OUT // BLOCK_ROWS
    order = jax.random.permutation(first, blocks)
    heavy = jnp.where(order < max(1, blocks // 16), 6.0, 1.0).astype(jnp.float32)
    row_scale = jnp.repeat(heavy, BLOCK_ROWS)
    base = scaled_field(second, D_OUT, D_IN)
    return (base * row_scale[:, None]).astype(jnp.float32)


def draw_right_factor(key, part):
    base = scaled_field(jax.random.fold_in(key, 23), D_IN, RANK)
    return (base / math.sqrt(D_IN)).astype(jnp.float32)


def draw_output_grads(key, part):
    base = scaled_field(jax.random.fold_in(key, 37), TOK, D_OUT)
    return (base / math.sqrt(TOK)).astype(jnp.bfloat16)


def draw_activations(key, part):
    base = scaled_field(jax.random.fold_in(key, 41), TOK, D_IN)
    return base.astype(jnp.bfloat16)


def level_of(key, extent, shards, smallest, largest):
    factor_of, own = 1.0, jax.random.fold_in(key, 6)
    for dim, shards_of in shards:
        steps = jnp.exp(jax.random.uniform(jax.random.fold_in(own, dim), (shards_of,), jnp.float32, smallest / len(shards), largest / len(shards)))
        factor_of = factor_of * jnp.repeat(steps, extent[dim] // shards_of).reshape([-1 if axis == dim else 1 for axis in range(len(extent))])
    return factor_of


def normal_values(own_key, dims, deviation, most, cuts=(), held_as=jnp.bfloat16):
    entries = deviation * jax.random.normal(own_key, dims, jnp.float32)
    if cuts:
        entries = entries * level_of(own_key, dims, cuts, -0.22, 0.18)
    return jnp.clip(entries, -most, most).astype(held_as)


def setup_inputs(seed: int = 0) -> dict:
    key_list = jax.random.split(jax.random.key(seed), 6)
    weight = normal_values(key_list[0], (D_OUT, D_IN), D_IN ** -0.5, 0.046875, ((0, 4), (1, 8)))
    momentum = draw_momentum(jax.random.fold_in(key_list[5], 71), 0)
    right_factor = draw_right_factor(jax.random.fold_in(key_list[5], 71), 0)
    output_grads = draw_output_grads(jax.random.fold_in(key_list[5], 71), 0)
    activations = draw_activations(jax.random.fold_in(key_list[5], 71), 0)
    return {"weight": weight, "momentum": momentum, "right_factor": right_factor, "output_grads": output_grads, "activations": activations}


FULL_PRECISION = lax.Precision.HIGHEST
MOMENTUM_DECAY = 0.95
LEARN_RATE = 0.002
NORM_EPS = 1e-06

def contract_rows(first, second):
    return lax.dot_general(first.astype(jnp.float32), second.astype(jnp.float32), (((0,), (0,)), ((), ())), precision=FULL_PRECISION, preferred_element_type=jnp.float32)

def outer_rows(first, second):
    return lax.dot_general(first.astype(jnp.float32), second.astype(jnp.float32), (((1,), (1,)), ((), ())), precision=FULL_PRECISION, preferred_element_type=jnp.float32)

def orthogonalize(left_factor, gram_matrix):
    lower_factor = jnp.linalg.cholesky(gram_matrix)
    identity = jnp.eye(gram_matrix.shape[0], dtype=gram_matrix.dtype)
    inverse = jax.scipy.linalg.solve_triangular(lower_factor, identity, lower=True)
    return outer_rows(left_factor, inverse)

def reference(weight, momentum, right_factor, output_grads, activations):
    grad_tile = lax.dot_general(output_grads.astype(jnp.float32), activations.astype(jnp.float32), (((0,), (0,)), ((), ())), preferred_element_type=jnp.float32)
    buffer = momentum + grad_tile
    left_factor = jnp.dot(buffer.astype(jnp.float32), right_factor.astype(jnp.float32), precision=FULL_PRECISION, preferred_element_type=jnp.float32)
    gram_matrix = contract_rows(left_factor, left_factor)
    ortho_left = orthogonalize(left_factor, gram_matrix)
    projected = contract_rows(buffer, ortho_left)
    column_norm = jnp.sqrt(lax.optimization_barrier(jnp.sum(projected * projected, axis=0)) + NORM_EPS)
    new_momentum = buffer - (1.0 - MOMENTUM_DECAY) * outer_rows(ortho_left, projected)
    new_factor = projected / column_norm
    step_scale = LEARN_RATE * math.sqrt(max(D_OUT, D_IN))
    new_weight = (weight.astype(jnp.float32) - step_scale * outer_rows(ortho_left, new_factor)).astype(jnp.bfloat16)
    return (new_weight, new_momentum, new_factor)
```

```python
import math

import jax
import jax.numpy as jnp
from jax import lax
from jax.experimental import pallas as pl
from jax.experimental.pallas import tpu as pltpu
from jax.sharding import PartitionSpec as P

FULL = lax.Precision.HIGHEST
HIGH = lax.Precision.HIGH
MOMENTUM_DECAY = 0.95
LEARN_RATE = 0.002
NORM_EPS = 1e-06
SIDE = 128
PANEL = 8


def dot(first, second, dims, precision=None):
    return lax.dot_general(
        first,
        second,
        (((dims[0],), (dims[1],)), ((), ())),
        precision=precision,
        preferred_element_type=jnp.float32,
    )


def full_dot(first, second, dims):
    return lax.dot_general(first, second, (((dims[0],), (dims[1],)), ((), ())), precision=FULL, preferred_element_type=jnp.float32)


def factor_kernel(gram_ref, inverse_ref, work, pair):
    size = gram_ref.shape[0]
    count = size // SIDE
    work[...] = gram_ref[...]
    inverse_ref[...] = jnp.zeros_like(inverse_ref)
    lane = lax.broadcasted_iota(jnp.int32, (PANEL, 2 * SIDE), 1)
    line = lax.broadcasted_iota(jnp.int32, (PANEL, 1), 0)
    eye = (lax.broadcasted_iota(jnp.int32, (SIDE, SIDE), 0) == lax.broadcasted_iota(jnp.int32, (SIDE, SIDE), 1)).astype(jnp.float32)

    def eliminate(step, carry):
        base = pl.multiple_of(step * PANEL, PANEL)
        rows = pair[pl.ds(base, PANEL), :]
        columns = [
            jnp.sum(jnp.where(lane == base + j, rows, 0.0), axis=1, keepdims=True)
            for j in range(PANEL)
        ]
        for j in range(PANEL):
            pivot = columns[j][j : j + 1, :]
            root = lax.rsqrt(pivot)
            root = root * (1.5 - 0.5 * pivot * root * root)
            below = jnp.where(line > j, columns[j] * root, 0.0)
            scaled = rows[j : j + 1, :] * root
            rows = jnp.where(line == j, scaled, rows - below * scaled)
            for i in range(j + 1, PANEL):
                columns[i] = columns[i] - below * (columns[i][j : j + 1, :] * root)
        pair[pl.ds(base, PANEL), :] = rows
        later = jnp.where(lane >= base + PANEL, rows, 0.0)[:, :SIDE]
        pair[...] = pair[...] - full_dot(later, rows, (0, 0))
        return carry

    for k in range(count):
        here = slice(k * SIDE, (k + 1) * SIDE)
        pair[:, :SIDE] = work[here, here]
        pair[:, SIDE:] = eye
        lax.fori_loop(0, SIDE // PANEL, eliminate, 0)
        diagonal = pair[:, SIDE:]
        inverse_ref[here, here] = diagonal
        if k:
            inverse_ref[here, : k * SIDE] = full_dot(diagonal, inverse_ref[here, : k * SIDE], (1, 0))
        if k + 1 < count:
            after = slice((k + 1) * SIDE, size)
            strip = full_dot(work[after, here], diagonal, (1, 1))
            work[after, after] = work[after, after] - full_dot(strip, strip, (1, 1))
            done = (k + 1) * SIDE
            inverse_ref[after, :done] = inverse_ref[after, :done] - full_dot(strip, inverse_ref[here, :done], (1, 0))


def inverse_factor(gram_matrix):
    size = gram_matrix.shape[0]
    return pl.pallas_call(
        factor_kernel,
        out_shape=jax.ShapeDtypeStruct(gram_matrix.shape, jnp.float32),
        in_specs=[pl.BlockSpec(memory_space=pltpu.VMEM)],
        out_specs=pl.BlockSpec(memory_space=pltpu.VMEM),
        scratch_shapes=[
            pltpu.VMEM((size, size), jnp.float32),
            pltpu.VMEM((SIDE, 2 * SIDE), jnp.float32),
        ],
        name="inverse_factor",
    )(gram_matrix)


def tie(value, *others):
    return lax.optimization_barrier((value,) + others)[0]


def low_bit(number):
    return number & -number


def children(number, size):
    bit = (low_bit(number) if number else size) // 2
    while bit:
        yield number | bit
        bit //= 2


def swap(block, axis, size, hop):
    return lax.ppermute(block, axis, [(i, i ^ hop) for i in range(size)])


def exchange_gather(block, axis, size, use=None):
    blocks, coming = {}, {0: block}
    order = sorted(range(size), key=lambda m: (bin(m).count("1"), -m))
    if size == 8:
        order = [0, 2, 1, 4, 3, 6, 5, 7]
    state = None
    for m in order:
        blocks[m] = coming[m] if state is None else tie(coming[m], *jax.tree.leaves(state))
        for child in children(m, size):
            coming[child] = swap(blocks[m], axis, size, low_bit(child))
        if use is not None:
            state = use(m, blocks[m], state)
    return blocks, state


def scatter_order(size):
    return sorted(range(1, size), key=lambda m: (low_bit(m), -m))


def exchange_scatter(parts, axis, size):
    parts = dict(parts)
    for m in scatter_order(size):
        hop = low_bit(m)
        parts[m ^ hop] = parts[m ^ hop] + swap(parts[m], axis, size, hop)
    return parts[0]


def assemble(blocks, index):
    size = len(blocks)
    first = blocks[0]
    whole = jnp.zeros((size,) + first.shape, first.dtype)
    for m in range(size):
        whole = lax.dynamic_update_index_in_dim(whole, blocks[m], index ^ m, 0)
    return whole.reshape((size * first.shape[0],) + first.shape[1:])


def butterfly_sum(value, axis, size):
    hop = 1
    while hop < size:
        value = value + swap(value, axis, size, hop)
        hop *= 2
    return value


def split(value):
    high = value.astype(jnp.bfloat16)
    low = (value - high.astype(jnp.float32)).astype(jnp.bfloat16)
    return high, low


def make_body(rows_n, cols_n, step_scale):
    def body(weight, momentum, right_factor, output_grads, activations):
        row = lax.axis_index("row")
        col = lax.axis_index("col")
        tile_rows, tile_cols = momentum.shape
        rank = right_factor.shape[1]
        momentum_blocks = momentum.reshape(cols_n, tile_rows // cols_n, tile_cols)

        def momentum_block(m):
            return lax.dynamic_index_in_dim(momentum_blocks, col ^ m, 0, keepdims=False)

        grads_own = lax.all_to_all(output_grads, "col", split_axis=1, concat_axis=0, tiled=True)
        factor_blocks, _ = exchange_gather(right_factor, "row", rows_n)
        factor = tie(assemble(factor_blocks, row), grads_own)

        parts, last = {}, None
        for m in scatter_order(cols_n) + [0]:
            operand = factor if last is None else tie(factor, last)
            last = parts[m] = lax.optimization_barrier(dot(momentum_block(m), operand, (1, 0), HIGH))
        token_part = dot(activations.astype(jnp.float32), factor, (1, 0), HIGH)
        token_sums = tie(lax.psum(token_part, "col"), last)
        token_sums = lax.all_gather(token_sums, "row", axis=0, tiled=True)
        left_own = exchange_scatter(parts, "col", cols_n)
        left_own = left_own + dot(grads_own.astype(jnp.float32), token_sums, (0, 0), HIGH)
        acts_own = lax.all_to_all(
            tie(activations, left_own), "row", split_axis=1, concat_axis=0, tiled=True
        )

        def use(m, block, state):
            product = dot(momentum_block(m), block, (0, 0), HIGH)
            gram = dot(block, block, (0, 0), FULL)
            if state is None:
                return product, gram
            return state[0] + product, state[1] + gram

        left_blocks, (product, gram) = exchange_gather(left_own, "col", cols_n, use)
        gram_matrix = butterfly_sum(gram, "row", rows_n)
        left_rows = assemble(left_blocks, col)
        token_left = butterfly_sum(
            dot(output_grads.astype(jnp.float32), left_rows, (1, 0), HIGH), "row", rows_n
        )

        product = product.reshape(rows_n, tile_cols // rows_n, rank)
        product_own = exchange_scatter(
            {
                m: lax.dynamic_index_in_dim(product, row ^ m, 0, keepdims=False)
                for m in range(rows_n)
            },
            "row",
            rows_n,
        )
        token_left = lax.all_gather(token_left, "col", axis=0, tiled=True)
        acts_whole = lax.all_gather(tie(activations, gram), "row", axis=0, tiled=True)
        grads_whole = lax.all_gather(tie(output_grads, gram), "col", axis=0, tiled=True)

        inverse = inverse_factor(gram_matrix)
        product_own = product_own + dot(acts_own.astype(jnp.float32), token_left, (0, 0), HIGH)
        projected_own = dot(product_own, inverse, (1, 1), FULL)
        squares = jnp.sum(projected_own * projected_own, axis=0, keepdims=True)
        squares = butterfly_sum(butterfly_sum(squares, "row", rows_n), "col", cols_n)
        column_norm = jnp.sqrt(squares + NORM_EPS)
        new_factor = projected_own / column_norm

        high_own, low_own = split(projected_own)
        projected_high = assemble(exchange_gather(high_own, "row", rows_n)[0], row)
        projected_low = assemble(exchange_gather(low_own, "row", rows_n)[0], row)

        ortho_left = dot(left_rows, inverse, (1, 1), HIGH)
        ortho_high = ortho_left.astype(jnp.bfloat16)
        buffer = momentum + dot(grads_whole, acts_whole, (0, 0))
        new_momentum = buffer - (1.0 - MOMENTUM_DECAY) * dot(ortho_high, projected_high, (1, 1))
        factor_cols = (
            projected_high.astype(jnp.float32) + projected_low.astype(jnp.float32)
        ) / column_norm
        new_weight = (
            weight.astype(jnp.float32) - step_scale * dot(ortho_left, factor_cols, (1, 1), HIGH)
        ).astype(jnp.bfloat16)
        return (new_weight, new_momentum, new_factor)

    return body


def solution(mesh):
    rows_n, cols_n = mesh.shape["row"], mesh.shape["col"]
    in_specs = (
        P("row", "col"),
        P("row", "col"),
        P(("col", "row"), None),
        P("col", "row"),
        P("row", "col"),
    )
    out_specs = (P("row", "col"), P("row", "col"), P(("col", "row"), None))

    def step(weight, momentum, right_factor, output_grads, activations):
        step_scale = LEARN_RATE * math.sqrt(max(weight.shape))
        return jax.shard_map(
            make_body(rows_n, cols_n, step_scale),
            mesh=mesh,
            in_specs=in_specs,
            out_specs=out_specs,
            check_vma=False,
        )(weight, momentum, right_factor, output_grads, activations)

    return step
```

```python
import math

import jax
import jax.numpy as jnp
from jax import lax
from jax.experimental import pallas as pl
from jax.experimental.pallas import tpu as pltpu
from jax.sharding import PartitionSpec as P

FULL = lax.Precision.HIGHEST
HIGH = lax.Precision.HIGH
MOMENTUM_DECAY = 0.95
LEARN_RATE = 0.002
NORM_EPS = 1e-06
SIDE = 128
PANEL = 8


def dot(first, second, dims, precision=None):
    return lax.dot_general(
        first,
        second,
        (((dims[0],), (dims[1],)), ((), ())),
        precision=precision,
        preferred_element_type=jnp.float32,
    )


def full_dot(first, second, dims):
    return lax.dot_general(first, second, (((dims[0],), (dims[1],)), ((), ())), precision=FULL, preferred_element_type=jnp.float32)


def factor_kernel(gram_ref, inverse_ref, work, pair):
    size = gram_ref.shape[0]
    count = size // SIDE
    work[...] = gram_ref[...]
    inverse_ref[...] = jnp.zeros_like(inverse_ref)
    lane = lax.broadcasted_iota(jnp.int32, (PANEL, 2 * SIDE), 1)
    line = lax.broadcasted_iota(jnp.int32, (PANEL, 1), 0)
    eye = (lax.broadcasted_iota(jnp.int32, (SIDE, SIDE), 0) == lax.broadcasted_iota(jnp.int32, (SIDE, SIDE), 1)).astype(jnp.float32)

    def eliminate(step, carry):
        base = pl.multiple_of(step * PANEL, PANEL)
        rows = pair[pl.ds(base, PANEL), :]
        columns = [
            jnp.sum(jnp.where(lane == base + j, rows, 0.0), axis=1, keepdims=True)
            for j in range(PANEL)
        ]
        for j in range(PANEL):
            pivot = columns[j][j : j + 1, :]
            root = lax.rsqrt(pivot)
            root = root * (1.5 - 0.5 * pivot * root * root)
            below = jnp.where(line > j, columns[j] * root, 0.0)
            scaled = rows[j : j + 1, :] * root
            rows = jnp.where(line == j, scaled, rows - below * scaled)
            for i in range(j + 1, PANEL):
                columns[i] = columns[i] - below * (columns[i][j : j + 1, :] * root)
        pair[pl.ds(base, PANEL), :] = rows
        later = jnp.where(lane >= base + PANEL, rows, 0.0)[:, :SIDE]
        pair[...] = pair[...] - full_dot(later, rows, (0, 0))
        return carry

    for k in range(count):
        here = slice(k * SIDE, (k + 1) * SIDE)
        pair[:, :SIDE] = work[here, here]
        pair[:, SIDE:] = eye
        lax.fori_loop(0, SIDE // PANEL, eliminate, 0)
        diagonal = pair[:, SIDE:]
        inverse_ref[here, here] = diagonal
        if k:
            inverse_ref[here, : k * SIDE] = full_dot(diagonal, inverse_ref[here, : k * SIDE], (1, 0))
        if k + 1 < count:
            after = slice((k + 1) * SIDE, size)
            strip = full_dot(work[after, here], diagonal, (1, 1))
            work[after, after] = work[after, after] - full_dot(strip, strip, (1, 1))
            done = (k + 1) * SIDE
            inverse_ref[after, :done] = inverse_ref[after, :done] - full_dot(strip, inverse_ref[here, :done], (1, 0))


def inverse_factor(gram_matrix):
    size = gram_matrix.shape[0]
    return pl.pallas_call(
        factor_kernel,
        out_shape=jax.ShapeDtypeStruct(gram_matrix.shape, jnp.float32),
        in_specs=[pl.BlockSpec(memory_space=pltpu.VMEM)],
        out_specs=pl.BlockSpec(memory_space=pltpu.VMEM),
        scratch_shapes=[
            pltpu.VMEM((size, size), jnp.float32),
            pltpu.VMEM((SIDE, 2 * SIDE), jnp.float32),
        ],
        name="inverse_factor",
    )(gram_matrix)


def momentum_kernel(old, grads_a, grads_b, acts_a, acts_b, ortho, projected, new):
    width = new.shape[1]
    step = min(512, width)
    for start in range(0, width, step):
        here = slice(start, start + step)
        total = dot(ortho[...], projected[here, :], (1, 1))
        total += dot(grads_a[...], acts_a[:, here], (0, 0))
        total += dot(grads_b[...], acts_b[:, here], (0, 0))
        new[:, here] = old[:, here] + total


def momentum_update(momentum, grads, acts, ortho, projected):
    height, width = momentum.shape
    rows = min(512, height)
    rank = ortho.shape[1]
    tokens = grads[0].shape[0]

    def whole(shape):
        return pl.BlockSpec(shape, lambda i: (0, 0))

    return pl.pallas_call(
        momentum_kernel,
        grid=(height // rows,),
        out_shape=jax.ShapeDtypeStruct(momentum.shape, jnp.float32),
        in_specs=[
            pl.BlockSpec((rows, width), lambda i: (i, 0)),
            pl.BlockSpec((tokens, rows), lambda i: (0, i)),
            pl.BlockSpec((tokens, rows), lambda i: (0, i)),
            whole((tokens, width)),
            whole((tokens, width)),
            pl.BlockSpec((rows, rank), lambda i: (i, 0)),
            whole((width, rank)),
        ],
        out_specs=pl.BlockSpec((rows, width), lambda i: (i, 0)),
        compiler_params=pltpu.CompilerParams(vmem_limit_bytes=60 * 1024 * 1024),
        cost_estimate=pl.CostEstimate(
            flops=2 * height * width * (2 * tokens + rank),
            bytes_accessed=8 * height * width,
            transcendentals=0,
        ),
        name="momentum_update",
    )(momentum, *grads, *acts, ortho, projected)


def meet(*values):
    return lax.optimization_barrier(values)


def low_bit(number):
    return number & -number


def children(number, size):
    bit = (low_bit(number) if number else size) // 2
    while bit:
        yield number | bit
        bit //= 2


def swap(block, axis, size, hop):
    return lax.ppermute(block, axis, [(i, i ^ hop) for i in range(size)])


def exchange_gather(block, axis, size, use=None, wire=None):
    blocks, coming = {}, {0: block if wire is None else pack(block, wire)}
    order = sorted(range(size), key=lambda m: (bin(m).count("1"), -m))
    if size == 8:
        order = [0, 2, 1, 4, 3, 6, 5, 7]
    state = None
    for m in order:
        blocks[m] = coming[m]
        if state is not None:
            blocks[m], *state = meet(coming[m], *state)
        for child in children(m, size):
            coming[child] = swap(blocks[m], axis, size, low_bit(child))
        if wire is not None:
            blocks[m] = unpack(blocks[m], wire)
        if use is not None:
            state = use(m, blocks[m], state)
    return blocks, state


def scatter_order(size):
    return sorted(range(1, size), key=lambda m: (low_bit(m), -m))


def exchange_scatter(parts, axis, size):
    parts = dict(parts)
    for m in scatter_order(size):
        hop = low_bit(m)
        parts[m ^ hop] = parts[m ^ hop] + swap(parts[m], axis, size, hop)
    return parts[0]


def paced_scatter(make, operand, axis, size, wire):
    leaves = sorted(range(1, size, 2), reverse=True)
    inner = sorted(range(2, size, 2), key=lambda m: (low_bit(m), -m))
    if size == 8:
        inner = [6, 4, 2]
    parts, arrived, last = {}, {}, None

    def send(m):
        arrived[m] = swap(pack(parts[m], wire), axis, size, low_bit(m))

    for place, m in enumerate(leaves + inner + [0]):
        if last is not None:
            operand, parts[last] = meet(operand, parts[last])
            if last % 2:
                send(last)
        if 0 <= place - 3 < len(leaves):
            behind = leaves[place - 3]
            operand, arrived[behind] = meet(operand, arrived[behind])
        parts[m] = make(m, operand)
        last = m
    operand, parts[last] = meet(operand, parts[last])
    for m in sorted(range(0, size, 2), key=lambda m: (low_bit(m) if m else size, -m)):
        parts[m] = parts[m] + unpack(arrived[m | 1], wire)
        for child in children(m, size):
            if child != m | 1:
                parts[m] = parts[m] + unpack(arrived[child], wire)
        if m:
            send(m)
    return parts[0], operand


def halving_sum(blocks, axis, size, index):
    hop = 1
    while hop < size:
        bit = (index // hop) % 2
        pairs = blocks.reshape((-1, 2) + blocks.shape[1:])
        mine = lax.dynamic_index_in_dim(pairs, bit, 1, keepdims=False)
        other = lax.dynamic_index_in_dim(pairs, 1 - bit, 1, keepdims=False)
        blocks = mine + swap(other, axis, size, hop)
        hop *= 2
    return blocks[0]


def pack(block, wire):
    return (block * wire).astype(jnp.float16)


def unpack(block, wire):
    return block.astype(jnp.float32) / wire


def butterfly_max(value, axis, size):
    hop = 1
    while hop < size:
        value = jnp.maximum(value, swap(value, axis, size, hop))
        hop *= 2
    return value


def magnitude(value):
    return jnp.max(jnp.abs(value.astype(jnp.float32)))


def assemble(blocks, index):
    size = len(blocks)
    first = blocks[0]
    whole = jnp.zeros((size,) + first.shape, first.dtype)
    for m in range(size):
        whole = lax.dynamic_update_index_in_dim(whole, blocks[m], index ^ m, 0)
    return whole.reshape((size * first.shape[0],) + first.shape[1:])


def butterfly_sum(value, axis, size):
    hop = 1
    while hop < size:
        value = value + swap(value, axis, size, hop)
        hop *= 2
    return value


def split(value):
    high = value.astype(jnp.bfloat16)
    low = (value - high.astype(jnp.float32)).astype(jnp.bfloat16)
    return high, low


def make_body(rows_n, cols_n, step_scale):
    def body(weight, momentum, right_factor, output_grads, activations):
        row = lax.axis_index("row")
        col = lax.axis_index("col")
        tile_rows, tile_cols = momentum.shape
        rank = right_factor.shape[1]
        momentum_blocks = momentum.reshape(cols_n, tile_rows // cols_n, tile_cols)

        def momentum_block(m):
            return lax.dynamic_index_in_dim(momentum_blocks, col ^ m, 0, keepdims=False)

        tokens = output_grads.shape[0]
        half = tokens // 2
        limits = jnp.stack([magnitude(v) for v in (momentum, right_factor, output_grads, activations)])
        limits = jnp.broadcast_to(limits[:, None], (4, 128))
        limits = butterfly_max(butterfly_max(limits, "row", rows_n), "col", cols_n)[:, 0]
        largest = (tile_cols * cols_n) * limits[1] * (
            limits[0] + (tokens * cols_n) * limits[2] * limits[3]
        )
        wire = 32768.0 / jnp.maximum(largest, 1e-30)

        grads_own = lax.all_to_all(output_grads, "col", split_axis=1, concat_axis=0, tiled=True)
        factor_blocks, _ = exchange_gather(right_factor, "row", rows_n)
        factor, grads_own = meet(assemble(factor_blocks, row), grads_own)
        grads_first = lax.all_gather(output_grads[:half], "col", axis=0, tiled=True)

        token_part = dot(activations.astype(jnp.float32), factor, (1, 0), HIGH)

        factor, token_part = meet(factor, token_part)

        def make(m, operand):
            return dot(momentum_block(m), operand, (1, 0), HIGH)

        token_share = halving_sum(
            token_part.reshape(cols_n, -1, rank), "col", cols_n, col
        )
        token_sums = lax.all_gather(token_share, ("row", "col"), axis=0, tiled=True)
        left_own, factor = paced_scatter(make, factor, "col", cols_n, wire)
        acts_whole, token_sums = meet(activations, token_sums)
        acts_whole = lax.all_gather(acts_whole, "row", axis=0, tiled=True)
        left_own = left_own + dot(grads_own.astype(jnp.float32), token_sums, (0, 0), HIGH)

        def use(m, block, state):
            product = dot(momentum_block(m), block, (0, 0), HIGH)
            gram = dot(block, block, (0, 0), FULL)
            if state is None:
                return [product, gram]
            return [state[0] + product, state[1] + gram]

        left_blocks, (product, gram) = exchange_gather(left_own, "col", cols_n, use, wire)
        grads_last, gram = meet(output_grads[half:], gram)
        gram_matrix = butterfly_sum(gram, "row", rows_n)
        left_rows = assemble(left_blocks, col)
        token_left = butterfly_sum(
            dot(output_grads.astype(jnp.float32), left_rows, (1, 0), HIGH), "row", rows_n
        )

        product = product.reshape(rows_n, tile_cols // rows_n, rank)
        product_own = exchange_scatter(
            {
                m: lax.dynamic_index_in_dim(product, row ^ m, 0, keepdims=False)
                for m in range(rows_n)
            },
            "row",
            rows_n,
        )
        token_left = lax.all_gather(token_left, "col", axis=0, tiled=True)
        grads_last = lax.all_gather(grads_last, "col", axis=0, tiled=True)
        acts_own = lax.dynamic_index_in_dim(
            acts_whole.reshape(-1, rows_n, tile_cols // rows_n), row, 1, keepdims=False
        )

        inverse = inverse_factor(gram_matrix)
        product_own = product_own + dot(acts_own.astype(jnp.float32), token_left, (0, 0), HIGH)
        projected_own = dot(product_own, inverse, (1, 1), FULL)

        high_own, low_own = split(projected_own)
        high_blocks, _ = exchange_gather(high_own, "row", rows_n)
        low_own, late_own, high_blocks[rows_n // 2] = meet(
            low_own, projected_own, high_blocks[rows_n // 2]
        )
        projected_high = assemble(high_blocks, row)
        projected_low = assemble(exchange_gather(low_own, "row", rows_n)[0], row)
        squares = jnp.sum(late_own * late_own, axis=0, keepdims=True)
        squares = butterfly_sum(butterfly_sum(squares, "row", rows_n), "col", cols_n)
        column_norm = jnp.sqrt(squares + NORM_EPS)
        new_factor = projected_own / column_norm

        ortho_left = dot(left_rows, inverse, (1, 1), HIGH)
        ortho_step = ((MOMENTUM_DECAY - 1.0) * ortho_left).astype(jnp.bfloat16)
        acts_parts = acts_whole.reshape(cols_n, 2, half, tile_cols)
        new_momentum = momentum_update(
            momentum,
            (grads_first, grads_last),
            (acts_parts[:, 0].reshape(-1, tile_cols), acts_parts[:, 1].reshape(-1, tile_cols)),
            ortho_step,
            projected_high,
        )
        factor_cols = (
            projected_high.astype(jnp.float32) + projected_low.astype(jnp.float32)
        ) / column_norm
        new_weight = (
            weight.astype(jnp.float32) - step_scale * dot(ortho_left, factor_cols, (1, 1), HIGH)
        ).astype(jnp.bfloat16)
        return (new_weight, new_momentum, new_factor)

    return body


def solution(mesh):
    rows_n, cols_n = mesh.shape["row"], mesh.shape["col"]
    in_specs = (
        P("row", "col"),
        P("row", "col"),
        P(("col", "row"), None),
        P("col", "row"),
        P("row", "col"),
    )
    out_specs = (P("row", "col"), P("row", "col"), P(("col", "row"), None))

    def step(weight, momentum, right_factor, output_grads, activations):
        step_scale = LEARN_RATE * math.sqrt(max(weight.shape))
        return jax.shard_map(
            make_body(rows_n, cols_n, step_scale),
            mesh=mesh,
            in_specs=in_specs,
            out_specs=out_specs,
            check_vma=False,
        )(weight, momentum, right_factor, output_grads, activations)

    return step
```

```python
import functools
import math

import jax
import jax.numpy as jnp
from jax import lax
from jax.experimental import pallas as pl
from jax.experimental.pallas import tpu as pltpu
from jax.sharding import PartitionSpec as P

FULL = lax.Precision.HIGHEST
HIGH = lax.Precision.HIGH
MOMENTUM_DECAY = 0.95
LEARN_RATE = 0.002
NORM_EPS = 1e-06
SIDE = 128
PANEL = 8


def dot(first, second, dims, precision=None):
    return lax.dot_general(
        first,
        second,
        (((dims[0],), (dims[1],)), ((), ())),
        precision=precision,
        preferred_element_type=jnp.float32,
    )


def full_dot(first, second, dims):
    return lax.dot_general(first, second, (((dims[0],), (dims[1],)), ((), ())), precision=FULL, preferred_element_type=jnp.float32)


def factor_kernel(gram_ref, inverse_ref, work, pair):
    size = gram_ref.shape[0]
    count = size // SIDE
    work[...] = gram_ref[...]
    inverse_ref[...] = jnp.zeros_like(inverse_ref)
    lane = lax.broadcasted_iota(jnp.int32, (PANEL, 2 * SIDE), 1)
    line = lax.broadcasted_iota(jnp.int32, (PANEL, 1), 0)
    eye = (lax.broadcasted_iota(jnp.int32, (SIDE, SIDE), 0) == lax.broadcasted_iota(jnp.int32, (SIDE, SIDE), 1)).astype(jnp.float32)

    def eliminate(step, carry):
        base = pl.multiple_of(step * PANEL, PANEL)
        rows = pair[pl.ds(base, PANEL), :]
        columns = [
            jnp.sum(jnp.where(lane == base + j, rows, 0.0), axis=1, keepdims=True)
            for j in range(PANEL)
        ]
        for j in range(PANEL):
            pivot = columns[j][j : j + 1, :]
            root = lax.rsqrt(pivot)
            root = root * (1.5 - 0.5 * pivot * root * root)
            below = jnp.where(line > j, columns[j] * root, 0.0)
            scaled = rows[j : j + 1, :] * root
            rows = jnp.where(line == j, scaled, rows - below * scaled)
            for i in range(j + 1, PANEL):
                columns[i] = columns[i] - below * (columns[i][j : j + 1, :] * root)
        pair[pl.ds(base, PANEL), :] = rows
        later = jnp.where(lane >= base + PANEL, rows, 0.0)[:, :SIDE]
        pair[...] = pair[...] - full_dot(later, rows, (0, 0))
        return carry

    for k in range(count):
        here = slice(k * SIDE, (k + 1) * SIDE)
        pair[:, :SIDE] = work[here, here]
        pair[:, SIDE:] = eye
        lax.fori_loop(0, SIDE // PANEL, eliminate, 0)
        diagonal = pair[:, SIDE:]
        inverse_ref[here, here] = diagonal
        if k:
            inverse_ref[here, : k * SIDE] = full_dot(diagonal, inverse_ref[here, : k * SIDE], (1, 0))
        if k + 1 < count:
            after = slice((k + 1) * SIDE, size)
            strip = full_dot(work[after, here], diagonal, (1, 1))
            work[after, after] = work[after, after] - full_dot(strip, strip, (1, 1))
            done = (k + 1) * SIDE
            inverse_ref[after, :done] = inverse_ref[after, :done] - full_dot(strip, inverse_ref[here, :done], (1, 0))


def inverse_factor(gram_matrix):
    size = gram_matrix.shape[0]
    return pl.pallas_call(
        factor_kernel,
        out_shape=jax.ShapeDtypeStruct(gram_matrix.shape, jnp.float32),
        in_specs=[pl.BlockSpec(memory_space=pltpu.VMEM)],
        out_specs=pl.BlockSpec(memory_space=pltpu.VMEM),
        scratch_shapes=[
            pltpu.VMEM((size, size), jnp.float32),
            pltpu.VMEM((SIDE, 2 * SIDE), jnp.float32),
        ],
        name="inverse_factor",
    )(gram_matrix)


def split(value):
    high = value.astype(jnp.bfloat16)
    low = (value - high.astype(jnp.float32)).astype(jnp.bfloat16)
    return high, low


def split_outside(value):
    high = lax.reduce_precision(value, 8, 7)
    return high.astype(jnp.bfloat16), (value - high).astype(jnp.bfloat16)


def part_kernel(place, old, high, low, out):
    first, rest = split(old[0])
    total = dot(first, high[0], (1, 0)) + dot(rest, high[0], (1, 0)) + dot(first, low[0], (1, 0))

    @pl.when(pl.program_id(0) == 0)
    def _():
        out[...] = total

    @pl.when(pl.program_id(0) > 0)
    def _():
        out[...] = out[...] + total


def part_product(place, blocks, high, low):
    _, height, width = blocks.shape
    count, depth, rank = high.shape
    return pl.pallas_call(
        part_kernel,
        grid_spec=pltpu.PrefetchScalarGridSpec(
            num_scalar_prefetch=1,
            grid=(count,),
            in_specs=[
                pl.BlockSpec((1, height, depth), lambda j, place: (place[0], 0, place[1] ^ j)),
                pl.BlockSpec((1, depth, rank), lambda j, place: (j, 0, 0)),
                pl.BlockSpec((1, depth, rank), lambda j, place: (j, 0, 0)),
            ],
            out_specs=pl.BlockSpec((height, rank), lambda j, place: (0, 0)),
        ),
        out_shape=jax.ShapeDtypeStruct((height, rank), jnp.float32),
        compiler_params=pltpu.CompilerParams(vmem_limit_bytes=32 * 1024 * 1024),
        cost_estimate=pl.CostEstimate(
            flops=6 * height * width * rank, bytes_accessed=4 * height * width, transcendentals=0
        ),
        name="part_product",
    )(place, blocks, high, low)


def step_kernel(started, place, block, old, grads, *refs):
    before, (product, small, high_t, low_t) = refs[:-4], refs[-4:]
    rank = block.shape[1]

    @pl.when(pl.program_id(0) == 0)
    def _():
        high, low = split(block[...])
        high_t[...] = high.T
        low_t[...] = low.T
        new_gram = (
            dot(high_t[...], high, (1, 0))
            + dot(high_t[...], low, (1, 0))
            + dot(low_t[...], high, (1, 0))
            + dot(low_t[...], low, (1, 0))
        )
        new_tokens = dot(grads[0], high, (1, 0)) + dot(grads[0], low, (1, 0))
        small[:rank] = before[1][:rank] + new_gram if started else new_gram
        small[rank:] = before[1][rank:] + new_tokens if started else new_tokens

    first, rest = split(old[0])
    total = (
        dot(high_t[...], first, (1, 0))
        + dot(low_t[...], first, (1, 0))
        + dot(high_t[...], rest, (1, 0))
    )
    product[0] = before[0][0] + total if started else total


def step_product(place, block, blocks, grads, before, chunk):
    _, height, width = blocks.shape
    rank = block.shape[1]
    tokens = grads.shape[1]
    started = before is not None
    shapes = [(width // chunk, rank, chunk), (rank + tokens, rank)]
    specs = [
        pl.BlockSpec((1, rank, chunk), lambda j, place: (j, 0, 0)),
        pl.BlockSpec((rank + tokens, rank), lambda j, place: (0, 0)),
    ]
    return pl.pallas_call(
        functools.partial(step_kernel, started),
        grid_spec=pltpu.PrefetchScalarGridSpec(
            num_scalar_prefetch=1,
            grid=(width // chunk,),
            in_specs=[
                pl.BlockSpec((height, rank), lambda j, place: (0, 0)),
                pl.BlockSpec((1, height, chunk), lambda j, place: (place[0], 0, j)),
                pl.BlockSpec((1, tokens, height), lambda j, place: (place[0], 0, 0)),
            ]
            + (specs if started else []),
            out_specs=specs,
            scratch_shapes=[
                pltpu.VMEM((rank, height), jnp.bfloat16),
                pltpu.VMEM((rank, height), jnp.bfloat16),
            ],
        ),
        out_shape=[jax.ShapeDtypeStruct(shape, jnp.float32) for shape in shapes],
        compiler_params=pltpu.CompilerParams(vmem_limit_bytes=40 * 1024 * 1024),
        cost_estimate=pl.CostEstimate(
            flops=6 * height * width * rank, bytes_accessed=4 * height * width, transcendentals=0
        ),
        name="step_product",
    )(place, block, blocks, grads, *(before or ()))


def momentum_kernel(old, grads_a, grads_b, acts, ortho, projected, new):
    width = new.shape[1]
    step = min(512, width)
    turned = ((MOMENTUM_DECAY - 1.0) * ortho[...]).astype(jnp.bfloat16)

    def fill(grads):
        for start in range(0, width, step):
            here = slice(start, start + step)
            total = dot(turned, projected[here, :], (1, 1))
            total += dot(grads[...], acts[:, here], (0, 0))
            new[:, here] = old[:, here] + total

    early = pl.program_id(0) < pl.num_programs(0) // 4
    pl.when(early)(lambda: fill(grads_a))
    pl.when(jnp.logical_not(early))(lambda: fill(grads_b))


def momentum_update(momentum, grads, acts, ortho, projected):
    height, width = momentum.shape
    rows = min(512, height // 4)
    count = height // rows
    rank = ortho.shape[1]
    tokens = acts.shape[0]

    def whole(shape):
        return pl.BlockSpec(shape, lambda i: (0, 0))

    return pl.pallas_call(
        momentum_kernel,
        grid=(count,),
        out_shape=jax.ShapeDtypeStruct(momentum.shape, jnp.float32),
        in_specs=[
            pl.BlockSpec((rows, width), lambda i: (i, 0)),
            pl.BlockSpec((tokens, rows), lambda i: (0, jnp.minimum(i, count // 4 - 1))),
            pl.BlockSpec((tokens, rows), lambda i: (0, jnp.maximum(i - count // 4, 0))),
            whole((tokens, width)),
            pl.BlockSpec((rows, rank), lambda i: (i, 0)),
            whole((width, rank)),
        ],
        out_specs=pl.BlockSpec((rows, width), lambda i: (i, 0)),
        compiler_params=pltpu.CompilerParams(vmem_limit_bytes=60 * 1024 * 1024),
        cost_estimate=pl.CostEstimate(
            flops=2 * height * width * (tokens + rank),
            bytes_accessed=8 * height * width,
            transcendentals=0,
        ),
        name="momentum_update",
    )(momentum, *grads, acts, ortho, projected)


def weight_kernel(step_scale, old, ortho, high, low, norm, new, factor_high, factor_low):
    @pl.when(pl.program_id(0) == 0)
    def _():
        factor = (high[...].astype(jnp.float32) + low[...].astype(jnp.float32)) / norm[...]
        factor_high[...], factor_low[...] = split(factor)

    width = new.shape[1]
    step = min(512, width)
    first, rest = split(ortho[...])
    for start in range(0, width, step):
        here = slice(start, start + step)
        total = dot(first, factor_high[here, :], (1, 1))
        total += dot(rest, factor_high[here, :], (1, 1))
        total += dot(first, factor_low[here, :], (1, 1))
        new[:, here] = (old[:, here].astype(jnp.float32) - step_scale * total).astype(new.dtype)


def weight_update(weight, ortho, high, low, norm, step_scale):
    height, width = weight.shape
    rows = min(512, height)
    rank = ortho.shape[1]

    def whole(shape):
        return pl.BlockSpec(shape, lambda i: (0, 0))

    return pl.pallas_call(
        functools.partial(weight_kernel, step_scale),
        grid=(height // rows,),
        out_shape=jax.ShapeDtypeStruct(weight.shape, weight.dtype),
        in_specs=[
            pl.BlockSpec((rows, width), lambda i: (i, 0)),
            pl.BlockSpec((rows, rank), lambda i: (i, 0)),
            whole((width, rank)),
            whole((width, rank)),
            whole((1, rank)),
        ],
        out_specs=pl.BlockSpec((rows, width), lambda i: (i, 0)),
        scratch_shapes=[pltpu.VMEM((width, rank), jnp.bfloat16)] * 2,
        compiler_params=pltpu.CompilerParams(vmem_limit_bytes=60 * 1024 * 1024),
        cost_estimate=pl.CostEstimate(
            flops=6 * height * width * rank, bytes_accessed=4 * height * width, transcendentals=0
        ),
        name="weight_update",
    )(weight, ortho, high, low, norm)


def meet(*values):
    return lax.optimization_barrier(values)


def low_bit(number):
    return number & -number


def children(number, size):
    bit = (low_bit(number) if number else size) // 2
    while bit:
        yield number | bit
        bit //= 2


def swap(block, axis, size, hop):
    return lax.ppermute(block, axis, [(i, i ^ hop) for i in range(size)])


def exchange_gather(block, axis, size, use=None, wire=None):
    blocks, coming = {}, {0: block if wire is None else pack(block, wire)}
    order = sorted(range(size), key=lambda m: (bin(m).count("1"), -m))
    if size == 8:
        order = [0, 2, 1, 4, 3, 6, 5, 7]
    state = None

    def receive(m):
        for child in children(m, size):
            coming[child] = swap(coming[m], axis, size, low_bit(child))
        blocks[m] = coming[m] if wire is None else unpack(coming[m], wire)

    receive(order[0])
    for place, m in enumerate(order):
        if use is None:
            if place:
                receive(m)
            continue
        if place == 1:
            coming[m], *state = meet(coming[m], *state)
            receive(m)
        if 0 < place < size - 1:
            later = order[place + 1]
            coming[later], *state = meet(coming[later], *state)
            receive(later)
        state = use(m, blocks[m], state)
    return blocks, state


def scatter_order(size):
    return sorted(range(1, size), key=lambda m: (low_bit(m), -m))


def exchange_scatter(parts, axis, size):
    parts = dict(parts)
    for m in scatter_order(size):
        hop = low_bit(m)
        parts[m ^ hop] = parts[m ^ hop] + swap(parts[m], axis, size, hop)
    return parts[0]


def paced_scatter(make, operand, axis, size, wire, beside):
    leaves = sorted(range(1, size, 2), reverse=True)
    inner = sorted(range(2, size, 2), key=lambda m: (low_bit(m), -m))
    if size == 8:
        inner = [6, 4, 2]
    parts, arrived, last = {}, {}, None

    def send(m):
        arrived[m] = swap(pack(parts[m], wire), axis, size, low_bit(m))

    for place, m in enumerate(leaves + inner + [0]):
        if last is not None:
            *operand, parts[last] = meet(*operand, parts[last])
            if last % 2:
                send(last)
        if 0 <= place - 3 < len(leaves):
            behind = leaves[place - 3]
            *operand, arrived[behind] = meet(*operand, arrived[behind])
        operand = beside(place, operand)
        parts[m] = make(m, operand)
        last = m
    *operand, parts[last] = meet(*operand, parts[last])
    for m in sorted(range(0, size, 2), key=lambda m: (low_bit(m) if m else size, -m)):
        parts[m] = parts[m] + unpack(arrived[m | 1], wire)
        for child in children(m, size):
            if child != m | 1:
                parts[m] = parts[m] + unpack(arrived[child], wire)
        if m:
            send(m)
    return parts[0], operand


def matrix_sum(value, axis, size, index):
    value = value + swap(value, axis, size, 1)
    mine = lax.dynamic_index_in_dim(
        value.reshape((2, -1) + value.shape[1:]), index % 2, 0, keepdims=False
    )
    hop = 2
    while hop < size:
        mine = mine + swap(mine, axis, size, hop)
        hop *= 2
    other = swap(mine, axis, size, 1)
    even = index % 2 == 0
    whole = jnp.concatenate([jnp.where(even, mine, other), jnp.where(even, other, mine)])
    return whole


class HalvingSum:
    def __init__(self, blocks, axis, size, index):
        self.blocks, self.axis, self.size, self.index = blocks, axis, size, index
        self.hop = 1

    def send(self):
        bit = (self.index // self.hop) % 2
        pairs = self.blocks.reshape((-1, 2) + self.blocks.shape[1:])
        self.mine = lax.dynamic_index_in_dim(pairs, bit, 1, keepdims=False)
        other = lax.dynamic_index_in_dim(pairs, 1 - bit, 1, keepdims=False)
        self.coming = swap(other, self.axis, self.size, self.hop)

    def receive(self, operand):
        *operand, self.coming = meet(*operand, self.coming)
        self.blocks = self.mine + self.coming
        self.hop *= 2
        if self.hop < self.size:
            self.send()
        return operand


def pack(block, wire):
    return (block * wire).astype(jnp.float16)


def unpack(block, wire):
    return block.astype(jnp.float32) / wire


def butterfly_max(value, axis, size):
    hop = 1
    while hop < size:
        value = jnp.maximum(value, swap(value, axis, size, hop))
        hop *= 2
    return value


def magnitude(value):
    return jnp.max(jnp.abs(value.astype(jnp.float32)))


def assemble(blocks, index):
    size = len(blocks)
    first = blocks[0]
    whole = jnp.zeros((size,) + first.shape, first.dtype)
    for m in range(size):
        whole = lax.dynamic_update_index_in_dim(whole, blocks[m], index ^ m, 0)
    return whole.reshape((size * first.shape[0],) + first.shape[1:])


def butterfly_sum(value, axis, size):
    hop = 1
    while hop < size:
        value = value + swap(value, axis, size, hop)
        hop *= 2
    return value


def make_body(rows_n, cols_n, step_scale):
    def body(weight, momentum, right_factor, output_grads, activations):
        row = lax.axis_index("row")
        col = lax.axis_index("col")
        tile_rows, tile_cols = momentum.shape
        rank = right_factor.shape[1]
        share = tile_rows // cols_n
        momentum_blocks = momentum.reshape(cols_n, share, tile_cols)

        tokens = output_grads.shape[0]
        limits = jnp.stack([magnitude(v) for v in (momentum, right_factor, output_grads, activations)])
        limits = jnp.broadcast_to(limits[:, None], (4, 128))
        limits = butterfly_max(butterfly_max(limits, "row", rows_n), "col", cols_n)[:, 0]
        largest = (tile_cols * cols_n) * limits[1] * (
            limits[0] + (tokens * cols_n) * limits[2] * limits[3]
        )
        wire = 32768.0 / jnp.maximum(largest, 1e-30)

        grads_blocks = output_grads.reshape(tokens, cols_n, share).transpose(1, 0, 2)
        grads_own = lax.all_to_all(grads_blocks, "col", split_axis=0, concat_axis=0, tiled=True)
        grads_own = grads_own.reshape(-1, share)
        grads_first = lax.all_gather(output_grads[:, : tile_rows // 4], "col", axis=0, tiled=True)
        factor_blocks, _ = exchange_gather(right_factor, "row", rows_n)
        wire, grads_own, *met = meet(
            wire, grads_own, *[factor_blocks[m] for m in range(rows_n)]
        )
        factor_blocks = dict(enumerate(met))
        factor = jnp.stack([factor_blocks[m] for m in range(rows_n)])
        factor_whole = assemble(factor_blocks, row)

        token_part = dot(activations.astype(jnp.float32), factor_whole, (1, 0), HIGH)
        factor, token_part = meet(factor, token_part)
        factor = split_outside(factor)

        def make(m, operand):
            if tile_cols // rows_n % 128:
                block = lax.dynamic_index_in_dim(momentum_blocks, col ^ m, 0, keepdims=False)
                return dot(block, factor_whole, (1, 0), HIGH)
            return part_product(jnp.stack([col ^ m, row]), momentum_blocks, *operand)

        token_parts = HalvingSum(token_part.reshape(cols_n, -1, rank), "col", cols_n, col)
        gathers = {}

        def beside(place, operand):
            if place == 0:
                token_parts.send()
            elif token_parts.hop < cols_n:
                operand = token_parts.receive(operand)
            if place == cols_n - 3:
                *operand, gathers["grads"], share_sum = meet(
                    *operand, grads_first, token_parts.blocks[0]
                )
                gathers["tokens"] = lax.all_gather(
                    share_sum, ("row", "col"), axis=0, tiled=True
                )
            return operand

        left_own, factor = paced_scatter(make, factor, "col", cols_n, wire, beside)
        left_own = left_own + dot(grads_own.astype(jnp.float32), gathers["tokens"], (0, 0), HIGH)
        left_own, acts_whole = meet(left_own, activations)
        acts_whole = lax.all_gather(acts_whole, "row", axis=0, tiled=True)

        chunk = min(512, tile_cols)

        def use(m, block, state):
            return step_product(
                jnp.stack([col ^ m]), block, momentum_blocks, grads_blocks, state, chunk
            )

        left_blocks, state = exchange_gather(left_own, "col", cols_n, use, wire)
        acts_whole, *state = meet(acts_whole, *state)
        product, small = state
        small = matrix_sum(small, "row", rows_n, row)
        gram_matrix, token_left = small[:rank], small[rank:]
        token_left = lax.all_gather(token_left, "col", axis=0, tiled=True)
        grads_last, gram_matrix = meet(output_grads[:, tile_rows // 4 :], gram_matrix)
        grads_last = lax.all_gather(grads_last, "col", axis=0, tiled=True)

        piece = tile_cols // rows_n

        def product_piece(m):
            if piece == chunk:
                return lax.dynamic_index_in_dim(product, row ^ m, 0, keepdims=False)
            whole = product.transpose(1, 0, 2).reshape(rank, tile_cols)
            return lax.dynamic_slice_in_dim(whole, (row ^ m) * piece, piece, 1)

        product_own = exchange_scatter({m: product_piece(m) for m in range(rows_n)}, "row", rows_n)
        acts_own = lax.dynamic_index_in_dim(
            acts_whole.reshape(-1, rows_n, piece), row, 1, keepdims=False
        )

        inverse = inverse_factor(gram_matrix)
        product_own = product_own + dot(token_left, acts_own.astype(jnp.float32), (0, 0), HIGH)
        projected_own = dot(product_own, inverse, (0, 1), FULL)

        high_own, low_own = split_outside(projected_own)
        high_blocks, _ = exchange_gather(high_own, "row", rows_n)
        high_blocks[1], projected_own = meet(high_blocks[1], projected_own)
        squares = jnp.sum(projected_own * projected_own, axis=0, keepdims=True)
        hops = [("row", rows_n, 1 << i) for i in range(rows_n.bit_length() - 1)]
        hops += [("col", cols_n, 1 << i) for i in range(cols_n.bit_length() - 1)]
        ortho_blocks = {}
        operand = inverse
        for m in range(cols_n):
            coming = swap(squares, *hops[m]) if m < len(hops) else None
            ortho_blocks[m] = dot(left_blocks[m], operand, (1, 1), HIGH)
            if coming is not None:
                coming, operand, ortho_blocks[m] = meet(coming, operand, ortho_blocks[m])
                squares = squares + coming
        column_norm = jnp.sqrt(squares + NORM_EPS)
        new_factor = projected_own / column_norm

        ortho_left = assemble(ortho_blocks, col)
        ortho_left, low_own, high_blocks[rows_n // 2] = meet(
            ortho_left, low_own, high_blocks[rows_n // 2]
        )
        projected_high = assemble(high_blocks, row)
        projected_low = assemble(exchange_gather(low_own, "row", rows_n)[0], row)

        new_weight = weight_update(
            weight, ortho_left, projected_high, projected_low, column_norm, step_scale
        )
        new_weight, grads_last = meet(new_weight, grads_last)
        new_momentum = momentum_update(
            momentum, (gathers["grads"], grads_last), acts_whole, ortho_left, projected_high
        )
        return (new_weight, new_momentum, new_factor)

    return body


def solution(mesh):
    rows_n, cols_n = mesh.shape["row"], mesh.shape["col"]
    in_specs = (
        P("row", "col"),
        P("row", "col"),
        P(("col", "row"), None),
        P("col", "row"),
        P("row", "col"),
    )
    out_specs = (P("row", "col"), P("row", "col"), P(("col", "row"), None))

    def step(weight, momentum, right_factor, output_grads, activations):
        step_scale = LEARN_RATE * math.sqrt(max(weight.shape))
        return jax.shard_map(
            make_body(rows_n, cols_n, step_scale),
            mesh=mesh,
            in_specs=in_specs,
            out_specs=out_specs,
            check_vma=False,
        )(weight, momentum, right_factor, output_grads, activations)

    return step
```

```python
import functools
import math

import jax
import jax.numpy as jnp
from jax import lax
from jax.experimental import pallas as pl
from jax.experimental.pallas import tpu as pltpu
from jax.sharding import PartitionSpec as P

FULL = lax.Precision.HIGHEST
HIGH = lax.Precision.HIGH
MOMENTUM_DECAY = 0.95
LEARN_RATE = 0.002
NORM_EPS = 1e-06
SIDE = 128
PANEL = 8


def dot(first, second, dims, precision=None):
    return lax.dot_general(
        first,
        second,
        (((dims[0],), (dims[1],)), ((), ())),
        precision=precision,
        preferred_element_type=jnp.float32,
    )


def full_dot(first, second, dims):
    return lax.dot_general(first, second, (((dims[0],), (dims[1],)), ((), ())), precision=FULL, preferred_element_type=jnp.float32)


def factor_kernel(gram_ref, inverse_ref, work, pair):
    size = gram_ref.shape[0]
    count = size // SIDE
    work[...] = gram_ref[...]
    inverse_ref[...] = jnp.zeros_like(inverse_ref)
    lane = lax.broadcasted_iota(jnp.int32, (PANEL, 2 * SIDE), 1)
    line = lax.broadcasted_iota(jnp.int32, (PANEL, 1), 0)
    eye = (lax.broadcasted_iota(jnp.int32, (SIDE, SIDE), 0) == lax.broadcasted_iota(jnp.int32, (SIDE, SIDE), 1)).astype(jnp.float32)

    def eliminate(step, carry):
        base = pl.multiple_of(step * PANEL, PANEL)
        rows = pair[pl.ds(base, PANEL), :]
        columns = [
            jnp.sum(jnp.where(lane == base + j, rows, 0.0), axis=1, keepdims=True)
            for j in range(PANEL)
        ]
        for j in range(PANEL):
            pivot = columns[j][j : j + 1, :]
            root = lax.rsqrt(pivot)
            root = root * (1.5 - 0.5 * pivot * root * root)
            below = jnp.where(line > j, columns[j] * root, 0.0)
            scaled = rows[j : j + 1, :] * root
            rows = jnp.where(line == j, scaled, rows - below * scaled)
            for i in range(j + 1, PANEL):
                columns[i] = columns[i] - below * (columns[i][j : j + 1, :] * root)
        pair[pl.ds(base, PANEL), :] = rows
        later = jnp.where(lane >= base + PANEL, rows, 0.0)[:, :SIDE]
        pair[...] = pair[...] - full_dot(later, rows, (0, 0))
        return carry

    for k in range(count):
        here = slice(k * SIDE, (k + 1) * SIDE)
        pair[:, :SIDE] = work[here, here]
        pair[:, SIDE:] = eye
        lax.fori_loop(0, SIDE // PANEL, eliminate, 0)
        diagonal = pair[:, SIDE:]
        inverse_ref[here, here] = diagonal
        if k:
            inverse_ref[here, : k * SIDE] = full_dot(diagonal, inverse_ref[here, : k * SIDE], (1, 0))
        if k + 1 < count:
            after = slice((k + 1) * SIDE, size)
            strip = full_dot(work[after, here], diagonal, (1, 1))
            work[after, after] = work[after, after] - full_dot(strip, strip, (1, 1))
            done = (k + 1) * SIDE
            inverse_ref[after, :done] = inverse_ref[after, :done] - full_dot(strip, inverse_ref[here, :done], (1, 0))


def inverse_factor(gram_matrix):
    size = gram_matrix.shape[0]
    return pl.pallas_call(
        factor_kernel,
        out_shape=jax.ShapeDtypeStruct(gram_matrix.shape, jnp.float32),
        in_specs=[pl.BlockSpec(memory_space=pltpu.VMEM)],
        out_specs=pl.BlockSpec(memory_space=pltpu.VMEM),
        scratch_shapes=[
            pltpu.VMEM((size, size), jnp.float32),
            pltpu.VMEM((SIDE, 2 * SIDE), jnp.float32),
        ],
        name="inverse_factor",
    )(gram_matrix)


def split(value):
    high = value.astype(jnp.bfloat16)
    low = (value - high.astype(jnp.float32)).astype(jnp.bfloat16)
    return high, low


def split_outside(value):
    high = lax.reduce_precision(value, 8, 7)
    return high.astype(jnp.bfloat16), (value - high).astype(jnp.bfloat16)


def part_kernel(place, old, high, low, out):
    first, rest = split(old[0])
    total = dot(first, high[0], (1, 0)) + dot(rest, high[0], (1, 0)) + dot(first, low[0], (1, 0))

    @pl.when(pl.program_id(0) == 0)
    def _():
        out[...] = total

    @pl.when(pl.program_id(0) > 0)
    def _():
        out[...] = out[...] + total


def part_product(place, blocks, high, low):
    _, height, width = blocks.shape
    count, depth, rank = high.shape
    return pl.pallas_call(
        part_kernel,
        grid_spec=pltpu.PrefetchScalarGridSpec(
            num_scalar_prefetch=1,
            grid=(count,),
            in_specs=[
                pl.BlockSpec((1, height, depth), lambda j, place: (place[0], 0, j)),
                pl.BlockSpec((1, depth, rank), lambda j, place: (j, 0, 0)),
                pl.BlockSpec((1, depth, rank), lambda j, place: (j, 0, 0)),
            ],
            out_specs=pl.BlockSpec((height, rank), lambda j, place: (0, 0)),
        ),
        out_shape=jax.ShapeDtypeStruct((height, rank), jnp.float32),
        compiler_params=pltpu.CompilerParams(vmem_limit_bytes=32 * 1024 * 1024),
        cost_estimate=pl.CostEstimate(
            flops=6 * height * width * rank, bytes_accessed=4 * height * width, transcendentals=0
        ),
        name="part_product",
    )(place, blocks, high, low)


def step_kernel(started, place, block, old, grads, *refs):
    before, (product, small, high_t, low_t) = refs[:-4], refs[-4:]
    rank = block.shape[1]

    @pl.when(pl.program_id(0) == 0)
    def _():
        high, low = split(block[...])
        high_t[...] = high.T
        low_t[...] = low.T
        new_gram = (
            dot(high_t[...], high, (1, 0))
            + dot(high_t[...], low, (1, 0))
            + dot(low_t[...], high, (1, 0))
            + dot(low_t[...], low, (1, 0))
        )
        new_tokens = dot(grads[0], high, (1, 0)) + dot(grads[0], low, (1, 0))
        small[:rank] = before[1][:rank] + new_gram if started else new_gram
        small[rank:] = before[1][rank:] + new_tokens if started else new_tokens

    first, rest = split(old[0])
    total = (
        dot(high_t[...], first, (1, 0))
        + dot(low_t[...], first, (1, 0))
        + dot(high_t[...], rest, (1, 0))
    )
    product[0] = before[0][0] + total if started else total


def step_product(place, block, blocks, grads, before, chunk):
    _, height, width = blocks.shape
    rank = block.shape[1]
    tokens = grads.shape[1]
    started = before is not None
    shapes = [(width // chunk, rank, chunk), (rank + tokens, rank)]
    specs = [
        pl.BlockSpec((1, rank, chunk), lambda j, place: (j, 0, 0)),
        pl.BlockSpec((rank + tokens, rank), lambda j, place: (0, 0)),
    ]
    return pl.pallas_call(
        functools.partial(step_kernel, started),
        grid_spec=pltpu.PrefetchScalarGridSpec(
            num_scalar_prefetch=1,
            grid=(width // chunk,),
            in_specs=[
                pl.BlockSpec((height, rank), lambda j, place: (0, 0)),
                pl.BlockSpec((1, height, chunk), lambda j, place: (place[0], 0, j)),
                pl.BlockSpec((1, tokens, height), lambda j, place: (place[0], 0, 0)),
            ]
            + (specs if started else []),
            out_specs=specs,
            scratch_shapes=[
                pltpu.VMEM((rank, height), jnp.bfloat16),
                pltpu.VMEM((rank, height), jnp.bfloat16),
            ],
        ),
        out_shape=[jax.ShapeDtypeStruct(shape, jnp.float32) for shape in shapes],
        compiler_params=pltpu.CompilerParams(vmem_limit_bytes=40 * 1024 * 1024),
        cost_estimate=pl.CostEstimate(
            flops=6 * height * width * rank, bytes_accessed=4 * height * width, transcendentals=0
        ),
        name="step_product",
    )(place, block, blocks, grads, *(before or ()))


def late_kernel(place, acts, tokens, base, out):
    high, low = split(tokens[...])
    out[...] = base[...] + dot(high, acts[...], (0, 0)) + dot(low, acts[...], (0, 0))


def late_product(place, acts, tokens, base):
    count, rank = tokens.shape
    width = base.shape[1]
    if width % 128:
        block = lax.dynamic_slice_in_dim(acts, place[0] * width, width, 1)
        return base + dot(tokens, block.astype(jnp.float32), (0, 0), HIGH)
    return pl.pallas_call(
        late_kernel,
        grid_spec=pltpu.PrefetchScalarGridSpec(
            num_scalar_prefetch=1,
            grid=(1,),
            in_specs=[
                pl.BlockSpec((count, width), lambda i, place: (0, place[0])),
                pl.BlockSpec((count, rank), lambda i, place: (0, 0)),
                pl.BlockSpec((rank, width), lambda i, place: (0, 0)),
            ],
            out_specs=pl.BlockSpec((rank, width), lambda i, place: (0, 0)),
        ),
        out_shape=jax.ShapeDtypeStruct((rank, width), jnp.float32),
        compiler_params=pltpu.CompilerParams(vmem_limit_bytes=40 * 1024 * 1024),
        cost_estimate=pl.CostEstimate(
            flops=4 * count * rank * width, bytes_accessed=6 * count * width, transcendentals=0
        ),
        name="late_product",
    )(place, acts, tokens, base)


def momentum_kernel(old, grads_a, grads_b, acts, ortho, projected, new):
    width = new.shape[1]
    step = min(512, width)
    turned = ((MOMENTUM_DECAY - 1.0) * ortho[...]).astype(jnp.bfloat16)

    def fill(grads):
        for start in range(0, width, step):
            here = slice(start, start + step)
            total = dot(turned, projected[here, :].astype(jnp.bfloat16), (1, 1))
            total += dot(grads[...], acts[:, here], (0, 0))
            new[:, here] = old[:, here] + total

    early = pl.program_id(0) < 3 * pl.num_programs(0) // 8
    pl.when(early)(lambda: fill(grads_a))
    pl.when(jnp.logical_not(early))(lambda: fill(grads_b))


def momentum_update(momentum, grads, acts, ortho, projected):
    height, width = momentum.shape
    rows = min(512, height // 8)
    count = height // rows
    first = 3 * count // 8
    rank = ortho.shape[1]
    tokens = acts.shape[0]

    def whole(shape):
        return pl.BlockSpec(shape, lambda i: (0, 0))

    return pl.pallas_call(
        momentum_kernel,
        grid=(count,),
        out_shape=jax.ShapeDtypeStruct(momentum.shape, jnp.float32),
        in_specs=[
            pl.BlockSpec((rows, width), lambda i: (i, 0)),
            pl.BlockSpec((tokens, rows), lambda i: (0, jnp.minimum(i, first - 1))),
            pl.BlockSpec((tokens, rows), lambda i: (0, jnp.maximum(i - first, 0))),
            whole((tokens, width)),
            pl.BlockSpec((rows, rank), lambda i: (i, 0)),
            whole((width, rank)),
        ],
        out_specs=pl.BlockSpec((rows, width), lambda i: (i, 0)),
        compiler_params=pltpu.CompilerParams(vmem_limit_bytes=60 * 1024 * 1024),
        cost_estimate=pl.CostEstimate(
            flops=2 * height * width * (tokens + rank),
            bytes_accessed=8 * height * width,
            transcendentals=0,
        ),
        name="momentum_update",
    )(momentum, *grads, acts, ortho, projected)


def weight_kernel(step_scale, old, ortho, projected, norm, new, factor_high, factor_low):
    @pl.when(pl.program_id(0) == 0)
    def _():
        factor_high[...], factor_low[...] = split(projected[...] / norm[...])

    width = new.shape[1]
    step = min(512, width)
    first, rest = split(ortho[...])
    for start in range(0, width, step):
        here = slice(start, start + step)
        total = dot(first, factor_high[here, :], (1, 1))
        total += dot(rest, factor_high[here, :], (1, 1))
        total += dot(first, factor_low[here, :], (1, 1))
        new[:, here] = (old[:, here].astype(jnp.float32) - step_scale * total).astype(new.dtype)


def weight_update(weight, ortho, projected, norm, step_scale):
    height, width = weight.shape
    rows = min(512, height)
    rank = ortho.shape[1]

    def whole(shape):
        return pl.BlockSpec(shape, lambda i: (0, 0))

    return pl.pallas_call(
        functools.partial(weight_kernel, step_scale),
        grid=(height // rows,),
        out_shape=jax.ShapeDtypeStruct(weight.shape, weight.dtype),
        in_specs=[
            pl.BlockSpec((rows, width), lambda i: (i, 0)),
            pl.BlockSpec((rows, rank), lambda i: (i, 0)),
            whole((width, rank)),
            whole((1, rank)),
        ],
        out_specs=pl.BlockSpec((rows, width), lambda i: (i, 0)),
        scratch_shapes=[pltpu.VMEM((width, rank), jnp.bfloat16)] * 2,
        compiler_params=pltpu.CompilerParams(vmem_limit_bytes=60 * 1024 * 1024),
        cost_estimate=pl.CostEstimate(
            flops=6 * height * width * rank, bytes_accessed=4 * height * width, transcendentals=0
        ),
        name="weight_update",
    )(weight, ortho, projected, norm)


def meet(*values):
    return lax.optimization_barrier(values)


def low_bit(number):
    return number & -number


def children(number, size):
    bit = (low_bit(number) if number else size) // 2
    while bit:
        yield number | bit
        bit //= 2


def swap(block, axis, size, hop):
    return lax.ppermute(block, axis, [(i, i ^ hop) for i in range(size)])


def exchange_gather(block, axis, size, use=None, wire=None, meanwhile=None):
    blocks, coming = {}, {0: block if wire is None else pack(block, wire)}
    order = sorted(range(size), key=lambda m: (bin(m).count("1"), -m))
    if size == 8:
        order = [0, 2, 1, 4, 3, 6, 5, 7]
    state = None

    def receive(m):
        for child in children(m, size):
            coming[child] = swap(coming[m], axis, size, low_bit(child))
        blocks[m] = coming[m] if wire is None else unpack(coming[m], wire)

    receive(order[0])
    if meanwhile is not None:
        coming[size // 2], *state = meet(coming[size // 2], *meanwhile())
    for place, m in enumerate(order):
        if use is None:
            if place:
                receive(m)
            continue
        if place == 1:
            coming[m], *state = meet(coming[m], *state)
            receive(m)
        if 0 < place < size - 1:
            later = order[place + 1]
            coming[later], *state = meet(coming[later], *state)
            receive(later)
        state = use(m, blocks[m], state)
    return blocks, state


def scatter_order(size):
    return sorted(range(1, size), key=lambda m: (low_bit(m), -m))


def paced_scatter(make, operand, axis, size, bounds, beside):
    leaves = sorted(range(1, size, 2), reverse=True)
    inner = sorted(range(2, size, 2), key=lambda m: (low_bit(m), -m))
    if size == 8:
        inner = [6, 4, 2]
    parts, arrived, last = {}, {}, None

    def level(m):
        return low_bit(m).bit_length() - 1

    def send(m):
        wire = scale_of(bounds.levels[level(m)])
        arrived[m] = swap(pack(parts[m], wire), axis, size, low_bit(m))

    def value(m):
        return unpack(arrived[m], scale_of(bounds.partners[level(m)]))

    for place, m in enumerate(leaves + inner + [0]):
        if last is not None:
            *operand, parts[last] = meet(*operand, parts[last])
            if last % 2:
                send(last)
        if 0 <= place - 3 < len(leaves):
            behind = leaves[place - 3]
            *operand, arrived[behind] = meet(*operand, arrived[behind])
        operand = beside(place, operand)
        parts[m] = make(m, operand)
        last = m
    *operand, parts[last] = meet(*operand, parts[last])
    for m in sorted(range(0, size, 2), key=lambda m: (low_bit(m) if m else size, -m)):
        parts[m] = parts[m] + value(m | 1)
        for child in children(m, size):
            if child != m | 1:
                parts[m] = parts[m] + value(child)
        if m:
            send(m)
    return parts[0], operand


def matrix_sum(value, axis, size, index, beside):
    value = value + swap(value, axis, size, 1)
    mine = lax.dynamic_index_in_dim(
        value.reshape((2, -1) + value.shape[1:]), index % 2, 0, keepdims=False
    )
    hop = 2
    while hop < size:
        coming = swap(mine, axis, size, hop)
        if hop == 2:
            coming, *held = meet(coming, *beside.values())
            beside = dict(zip(beside, held))
        mine = mine + coming
        hop *= 2
    other = swap(mine, axis, size, 1)
    even = index % 2 == 0
    whole = jnp.concatenate([jnp.where(even, mine, other), jnp.where(even, other, mine)])
    return whole, beside


class HalvingSum:
    def __init__(self, blocks, axis, size, index):
        self.blocks, self.axis, self.size, self.index = blocks, axis, size, index
        self.hop = 1

    def send(self):
        bit = (self.index // self.hop) % 2
        pairs = self.blocks.reshape((-1, 2) + self.blocks.shape[1:])
        self.mine = lax.dynamic_index_in_dim(pairs, bit, 1, keepdims=False)
        other = lax.dynamic_index_in_dim(pairs, 1 - bit, 1, keepdims=False)
        self.coming = swap(other, self.axis, self.size, self.hop)

    def receive(self, operand):
        *operand, self.coming = meet(*operand, self.coming)
        self.blocks = self.mine + self.coming
        self.hop *= 2
        if self.hop < self.size:
            self.send()
        return operand


def pack(block, wire):
    return (block * wire).astype(jnp.float16)


def unpack(block, wire):
    return block.astype(jnp.float32) / wire


class Bounds:
    def __init__(self, own, extra, axis, size):
        self.levels, self.partners = [jnp.broadcast_to(own, (1, 128))], []
        self.extra = jnp.broadcast_to(extra, (1, 128))
        self.axis, self.size = axis, size

    def send(self):
        message = jnp.concatenate([self.levels[-1], self.extra])
        self.coming = swap(message, self.axis, self.size, 1 << len(self.partners))

    def receive(self, operand):
        *operand, self.coming = meet(*operand, self.coming)
        self.partners.append(self.coming[:1])
        self.levels.append(self.levels[-1] + self.coming[:1])
        self.extra = jnp.maximum(self.extra, self.coming[1:])
        if 1 << len(self.partners) < self.size:
            self.send()
        return operand


def scale_of(bound):
    return 32768.0 / jnp.maximum(bound[0, 0], 1e-30)


def magnitude(value):
    return jnp.max(jnp.abs(value.astype(jnp.float32)))


def assemble(blocks, index):
    size = len(blocks)
    first = blocks[0]
    whole = jnp.zeros((size,) + first.shape, first.dtype)
    for m in range(size):
        whole = lax.dynamic_update_index_in_dim(whole, blocks[m], index ^ m, 0)
    return whole.reshape((size * first.shape[0],) + first.shape[1:])


def make_body(rows_n, cols_n, step_scale):
    def body(weight, momentum, right_factor, output_grads, activations):
        row = lax.axis_index("row")
        col = lax.axis_index("col")
        tile_rows, tile_cols = momentum.shape
        rank = right_factor.shape[1]
        share = tile_rows // cols_n
        momentum_blocks = momentum.reshape(cols_n, share, tile_cols)

        tokens = output_grads.shape[0]
        grads_blocks = output_grads.reshape(tokens, cols_n, share).transpose(1, 0, 2)
        grads_own = lax.all_to_all(grads_blocks, "col", split_axis=0, concat_axis=0, tiled=True)
        grads_own = grads_own.reshape(-1, share)
        factor_blocks, (largest,) = exchange_gather(
            right_factor, "row", rows_n, meanwhile=lambda: [magnitude(momentum)]
        )
        largest, grads_own, *met = meet(
            largest, grads_own, *[factor_blocks[m] for m in range(rows_n)]
        )
        factor_whole = assemble(dict(enumerate(met)), row)

        token_part = dot(activations.astype(jnp.float32), factor_whole, (1, 0), HIGH)
        factor_whole, token_part = meet(factor_whole, token_part)
        bounds = Bounds(
            tile_cols * largest * magnitude(factor_whole), magnitude(output_grads), "col", cols_n
        )
        depth = min(512, tile_cols)
        factor = [v.reshape(-1, depth, rank) for v in split_outside(factor_whole)]

        def make(m, operand):
            return part_product(jnp.stack([col ^ m]), momentum_blocks, *operand)

        token_parts = HalvingSum(token_part.reshape(cols_n, -1, rank), "col", cols_n, col)
        gathers = {}

        def beside(place, operand):
            if place == 0:
                token_parts.send()
                bounds.send()
            elif token_parts.hop < cols_n:
                operand = token_parts.receive(operand)
                operand = bounds.receive(operand)
                if token_parts.hop == cols_n:
                    gathers["tokens"] = lax.all_gather(
                        token_parts.blocks[0], ("row", "col"), axis=0, tiled=True
                    )
            return operand

        left_own, factor = paced_scatter(make, factor, "col", cols_n, bounds, beside)
        token_sums = gathers["tokens"]
        left_own = left_own + dot(grads_own.astype(jnp.float32), token_sums, (0, 0), HIGH)
        wire = scale_of(
            bounds.levels[-1] + (tokens * cols_n) * bounds.extra * magnitude(token_sums)
        )
        left_own, acts_whole = meet(left_own, activations)
        acts_whole = lax.all_gather(acts_whole, "row", axis=0, tiled=True)

        chunk = min(512, tile_cols)

        seen = []

        def use(m, block, state):
            if len(seen) == 2:
                *state, gathers["acts"], grads_first = meet(
                    *state, acts_whole, output_grads[:, : 3 * tile_rows // 8]
                )
                gathers["grads"] = lax.all_gather(grads_first, "col", axis=0, tiled=True)
            seen.append(m)
            return step_product(
                jnp.stack([col ^ m]), block, momentum_blocks, grads_blocks, state, chunk
            )

        left_blocks, state = exchange_gather(left_own, "col", cols_n, use, wire)
        acts_whole = gathers["acts"]
        product, small = state
        piece = tile_cols // rows_n

        def product_piece(m):
            if piece == chunk:
                return lax.dynamic_index_in_dim(product, row ^ m, 0, keepdims=False)
            whole = product.transpose(1, 0, 2).reshape(rank, tile_cols)
            return lax.dynamic_slice_in_dim(whole, (row ^ m) * piece, piece, 1)

        pieces = {m: product_piece(m) for m in range(rows_n)}
        pieces = {m: pieces[m] + swap(pieces[m | 1], "row", rows_n, 1) for m in range(0, rows_n, 2)}
        small, pieces = matrix_sum(small, "row", rows_n, row, pieces)
        gram_matrix, token_left = small[:rank], small[rank:]
        token_left, gathers["grads"] = meet(token_left, gathers["grads"])
        token_left = lax.all_gather(token_left, "col", axis=0, tiled=True)
        for m in sorted(range(2, rows_n, 2), key=lambda m: (low_bit(m), -m)):
            hop = low_bit(m)
            pieces[m ^ hop] = pieces[m ^ hop] + swap(pieces[m], "row", rows_n, hop)
        grads_last, gram_matrix = meet(output_grads[:, 3 * tile_rows // 8 :], gram_matrix)
        grads_last = lax.all_gather(grads_last, "col", axis=0, tiled=True)

        inverse = inverse_factor(gram_matrix)
        product_own = late_product(jnp.stack([row]), acts_whole, token_left, pieces[0])
        projected_own = dot(product_own, inverse, (0, 1), FULL)

        squares = jnp.sum(projected_own * projected_own, axis=0, keepdims=True)
        hops = [("row", rows_n, 1 << i) for i in range(rows_n.bit_length() - 1)]
        hops += [("col", cols_n, 1 << i) for i in range(cols_n.bit_length() - 1)]
        def meanwhile():
            sums, operand, blocks = squares, inverse, {}
            for m in range(cols_n):
                coming = swap(sums, *hops[m]) if m < len(hops) else None
                blocks[m] = dot(left_blocks[m], operand, (1, 1), HIGH)
                if coming is not None:
                    coming, operand, blocks[m] = meet(coming, operand, blocks[m])
                    sums = sums + coming
            return [assemble(blocks, col), sums]

        projected_blocks, (ortho_left, squares) = exchange_gather(
            projected_own, "row", rows_n, meanwhile=meanwhile
        )
        projected = assemble(projected_blocks, row)
        column_norm = jnp.sqrt(squares + NORM_EPS)
        new_factor = projected_own / column_norm

        new_weight = weight_update(
            weight, ortho_left, projected, column_norm, step_scale
        )
        new_weight, grads_last = meet(new_weight, grads_last)
        new_momentum = momentum_update(
            momentum, (gathers["grads"], grads_last), acts_whole, ortho_left, projected
        )
        return (new_weight, new_momentum, new_factor)

    return body


def solution(mesh):
    rows_n, cols_n = mesh.shape["row"], mesh.shape["col"]
    in_specs = (
        P("row", "col"),
        P("row", "col"),
        P(("col", "row"), None),
        P("col", "row"),
        P("row", "col"),
    )
    out_specs = (P("row", "col"), P("row", "col"), P(("col", "row"), None))

    def step(weight, momentum, right_factor, output_grads, activations):
        step_scale = LEARN_RATE * math.sqrt(max(weight.shape))
        return jax.shard_map(
            make_body(rows_n, cols_n, step_scale),
            mesh=mesh,
            in_specs=in_specs,
            out_specs=out_specs,
            check_vma=False,
        )(weight, momentum, right_factor, output_grads, activations)

    return step
```

```python
import functools
import math

import jax
import jax.numpy as jnp
from jax import lax
from jax.experimental import pallas as pl
from jax.experimental.pallas import tpu as pltpu
from jax.sharding import PartitionSpec as P

FULL = lax.Precision.HIGHEST
HIGH = lax.Precision.HIGH
MOMENTUM_DECAY = 0.95
LEARN_RATE = 0.002
NORM_EPS = 1e-06
SIDE = 128
PANEL = 8


def dot(first, second, dims, precision=None):
    return lax.dot_general(
        first,
        second,
        (((dims[0],), (dims[1],)), ((), ())),
        precision=precision,
        preferred_element_type=jnp.float32,
    )


def full_dot(first, second, dims):
    return lax.dot_general(first, second, (((dims[0],), (dims[1],)), ((), ())), precision=FULL, preferred_element_type=jnp.float32)


def factor_kernel(gram_ref, inverse_ref, work, pair):
    size = gram_ref.shape[0]
    count = size // SIDE
    work[...] = gram_ref[...]
    inverse_ref[...] = jnp.zeros_like(inverse_ref)
    lane = lax.broadcasted_iota(jnp.int32, (PANEL, 2 * SIDE), 1)
    line = lax.broadcasted_iota(jnp.int32, (PANEL, 1), 0)
    eye = (lax.broadcasted_iota(jnp.int32, (SIDE, SIDE), 0) == lax.broadcasted_iota(jnp.int32, (SIDE, SIDE), 1)).astype(jnp.float32)

    def eliminate(step, carry):
        base = pl.multiple_of(step * PANEL, PANEL)
        rows = pair[pl.ds(base, PANEL), :]
        columns = [
            jnp.sum(jnp.where(lane == base + j, rows, 0.0), axis=1, keepdims=True)
            for j in range(PANEL)
        ]
        for j in range(PANEL):
            pivot = columns[j][j : j + 1, :]
            root = lax.rsqrt(pivot)
            root = root * (1.5 - 0.5 * pivot * root * root)
            below = jnp.where(line > j, columns[j] * root, 0.0)
            scaled = rows[j : j + 1, :] * root
            rows = jnp.where(line == j, scaled, rows - below * scaled)
            for i in range(j + 1, PANEL):
                columns[i] = columns[i] - below * (columns[i][j : j + 1, :] * root)
        pair[pl.ds(base, PANEL), :] = rows
        later = jnp.where(lane >= base + PANEL, rows, 0.0)[:, :SIDE]
        pair[...] = pair[...] - full_dot(later, rows, (0, 0))
        return carry

    for k in range(count):
        here = slice(k * SIDE, (k + 1) * SIDE)
        pair[:, :SIDE] = work[here, here]
        pair[:, SIDE:] = eye
        lax.fori_loop(0, SIDE // PANEL, eliminate, 0)
        diagonal = pair[:, SIDE:]
        inverse_ref[here, here] = diagonal
        if k:
            inverse_ref[here, : k * SIDE] = full_dot(diagonal, inverse_ref[here, : k * SIDE], (1, 0))
        if k + 1 < count:
            after = slice((k + 1) * SIDE, size)
            strip = full_dot(work[after, here], diagonal, (1, 1))
            work[after, after] = work[after, after] - full_dot(strip, strip, (1, 1))
            done = (k + 1) * SIDE
            inverse_ref[after, :done] = inverse_ref[after, :done] - full_dot(strip, inverse_ref[here, :done], (1, 0))


def inverse_factor(gram_matrix):
    size = gram_matrix.shape[0]
    return pl.pallas_call(
        factor_kernel,
        out_shape=jax.ShapeDtypeStruct(gram_matrix.shape, jnp.float32),
        in_specs=[pl.BlockSpec(memory_space=pltpu.VMEM)],
        out_specs=pl.BlockSpec(memory_space=pltpu.VMEM),
        scratch_shapes=[
            pltpu.VMEM((size, size), jnp.float32),
            pltpu.VMEM((SIDE, 2 * SIDE), jnp.float32),
        ],
        name="inverse_factor",
    )(gram_matrix)


def split(value):
    high = value.astype(jnp.bfloat16)
    low = (value - high.astype(jnp.float32)).astype(jnp.bfloat16)
    return high, low


def split_outside(value):
    high = lax.reduce_precision(value, 8, 7)
    return high.astype(jnp.bfloat16), (value - high).astype(jnp.bfloat16)


def part_kernel(place, old, high, low, out):
    first, rest = split(old[0])
    total = dot(first, high[0], (1, 0)) + dot(rest, high[0], (1, 0)) + dot(first, low[0], (1, 0))

    @pl.when(pl.program_id(0) == 0)
    def _():
        out[...] = total

    @pl.when(pl.program_id(0) > 0)
    def _():
        out[...] = out[...] + total


def part_product(place, blocks, high, low):
    _, height, width = blocks.shape
    count, depth, rank = high.shape
    return pl.pallas_call(
        part_kernel,
        grid_spec=pltpu.PrefetchScalarGridSpec(
            num_scalar_prefetch=1,
            grid=(count,),
            in_specs=[
                pl.BlockSpec((1, height, depth), lambda j, place: (place[0], 0, j)),
                pl.BlockSpec((1, depth, rank), lambda j, place: (j, 0, 0)),
                pl.BlockSpec((1, depth, rank), lambda j, place: (j, 0, 0)),
            ],
            out_specs=pl.BlockSpec((height, rank), lambda j, place: (0, 0)),
        ),
        out_shape=jax.ShapeDtypeStruct((height, rank), jnp.float32),
        compiler_params=pltpu.CompilerParams(vmem_limit_bytes=32 * 1024 * 1024),
        cost_estimate=pl.CostEstimate(
            flops=6 * height * width * rank, bytes_accessed=4 * height * width, transcendentals=0
        ),
        name="part_product",
    )(place, blocks, high, low)


def step_kernel(started, place, block, old, grads, *refs):
    before, (product, small, high_t, low_t) = refs[:-4], refs[-4:]
    rank = block.shape[1]

    @pl.when(pl.program_id(0) == 0)
    def _():
        high, low = split(block[...])
        high_t[...] = high.T
        low_t[...] = low.T
        new_gram = (
            dot(high_t[...], high, (1, 0))
            + dot(high_t[...], low, (1, 0))
            + dot(low_t[...], high, (1, 0))
            + dot(low_t[...], low, (1, 0))
        )
        new_tokens = dot(grads[0], high, (1, 0)) + dot(grads[0], low, (1, 0))
        small[:rank] = before[1][:rank] + new_gram if started else new_gram
        small[rank:] = before[1][rank:] + new_tokens if started else new_tokens

    first, rest = split(old[0])
    total = (
        dot(high_t[...], first, (1, 0))
        + dot(low_t[...], first, (1, 0))
        + dot(high_t[...], rest, (1, 0))
    )
    product[0] = before[0][0] + total if started else total


def step_product(place, block, blocks, grads, before, chunk):
    _, height, width = blocks.shape
    rank = block.shape[1]
    tokens = grads.shape[1]
    started = before is not None
    shapes = [(width // chunk, rank, chunk), (rank + tokens, rank)]
    specs = [
        pl.BlockSpec((1, rank, chunk), lambda j, place: (j, 0, 0)),
        pl.BlockSpec((rank + tokens, rank), lambda j, place: (0, 0)),
    ]
    return pl.pallas_call(
        functools.partial(step_kernel, started),
        grid_spec=pltpu.PrefetchScalarGridSpec(
            num_scalar_prefetch=1,
            grid=(width // chunk,),
            in_specs=[
                pl.BlockSpec((height, rank), lambda j, place: (0, 0)),
                pl.BlockSpec((1, height, chunk), lambda j, place: (place[0], 0, j)),
                pl.BlockSpec((1, tokens, height), lambda j, place: (place[0], 0, 0)),
            ]
            + (specs if started else []),
            out_specs=specs,
            scratch_shapes=[
                pltpu.VMEM((rank, height), jnp.bfloat16),
                pltpu.VMEM((rank, height), jnp.bfloat16),
            ],
        ),
        out_shape=[jax.ShapeDtypeStruct(shape, jnp.float32) for shape in shapes],
        compiler_params=pltpu.CompilerParams(vmem_limit_bytes=40 * 1024 * 1024),
        cost_estimate=pl.CostEstimate(
            flops=6 * height * width * rank, bytes_accessed=4 * height * width, transcendentals=0
        ),
        input_output_aliases={4: 0, 5: 1} if started else {},
        name="step_product",
    )(place, block, blocks, grads, *(before or ()))


def late_kernel(place, acts, tokens, base, out):
    high, low = split(tokens[...])
    out[...] = base[...] + dot(high, acts[...], (0, 0)) + dot(low, acts[...], (0, 0))


def late_product(place, acts, tokens, base):
    count, rank = tokens.shape
    width = base.shape[1]
    if width % 128:
        block = lax.dynamic_slice_in_dim(acts, place[0] * width, width, 1)
        return base + dot(tokens, block.astype(jnp.float32), (0, 0), HIGH)
    return pl.pallas_call(
        late_kernel,
        grid_spec=pltpu.PrefetchScalarGridSpec(
            num_scalar_prefetch=1,
            grid=(1,),
            in_specs=[
                pl.BlockSpec((count, width), lambda i, place: (0, place[0])),
                pl.BlockSpec((count, rank), lambda i, place: (0, 0)),
                pl.BlockSpec((rank, width), lambda i, place: (0, 0)),
            ],
            out_specs=pl.BlockSpec((rank, width), lambda i, place: (0, 0)),
        ),
        out_shape=jax.ShapeDtypeStruct((rank, width), jnp.float32),
        compiler_params=pltpu.CompilerParams(vmem_limit_bytes=40 * 1024 * 1024),
        cost_estimate=pl.CostEstimate(
            flops=4 * count * rank * width, bytes_accessed=6 * count * width, transcendentals=0
        ),
        name="late_product",
    )(place, acts, tokens, base)


def momentum_kernel(old, grads_a, grads_b, acts, ortho, projected, new):
    width = new.shape[1]
    step = min(512, width)
    turned = ((MOMENTUM_DECAY - 1.0) * ortho[...]).astype(jnp.bfloat16)

    def fill(grads):
        for start in range(0, width, step):
            here = slice(start, start + step)
            total = dot(turned, projected[here, :].astype(jnp.bfloat16), (1, 1))
            total += dot(grads[...], acts[:, here], (0, 0))
            new[:, here] = old[:, here] + total

    early = pl.program_id(0) < 3 * pl.num_programs(0) // 8
    pl.when(early)(lambda: fill(grads_a))
    pl.when(jnp.logical_not(early))(lambda: fill(grads_b))


def momentum_update(momentum, grads, acts, ortho, projected):
    height, width = momentum.shape
    rows = min(512, height // 8)
    count = height // rows
    first = 3 * count // 8
    rank = ortho.shape[1]
    tokens = acts.shape[0]

    def whole(shape):
        return pl.BlockSpec(shape, lambda i: (0, 0))

    return pl.pallas_call(
        momentum_kernel,
        grid=(count,),
        out_shape=jax.ShapeDtypeStruct(momentum.shape, jnp.float32),
        in_specs=[
            pl.BlockSpec((rows, width), lambda i: (i, 0)),
            pl.BlockSpec((tokens, rows), lambda i: (0, jnp.minimum(i, first - 1))),
            pl.BlockSpec((tokens, rows), lambda i: (0, jnp.maximum(i - first, 0))),
            whole((tokens, width)),
            pl.BlockSpec((rows, rank), lambda i: (i, 0)),
            whole((width, rank)),
        ],
        out_specs=pl.BlockSpec((rows, width), lambda i: (i, 0)),
        compiler_params=pltpu.CompilerParams(vmem_limit_bytes=60 * 1024 * 1024),
        cost_estimate=pl.CostEstimate(
            flops=2 * height * width * (tokens + rank),
            bytes_accessed=8 * height * width,
            transcendentals=0,
        ),
        name="momentum_update",
    )(momentum, *grads, acts, ortho, projected)


def weight_kernel(step_scale, old, ortho, projected, norm, new, factor_high, factor_low):
    @pl.when(pl.program_id(0) == 0)
    def _():
        factor_high[...], factor_low[...] = split(projected[...] / norm[...])

    width = new.shape[1]
    step = min(512, width)
    first, rest = split(ortho[...])
    for start in range(0, width, step):
        here = slice(start, start + step)
        total = dot(first, factor_high[here, :], (1, 1))
        total += dot(rest, factor_high[here, :], (1, 1))
        total += dot(first, factor_low[here, :], (1, 1))
        new[:, here] = (old[:, here].astype(jnp.float32) - step_scale * total).astype(new.dtype)


def weight_update(weight, ortho, projected, norm, step_scale):
    height, width = weight.shape
    rows = min(512, height)
    rank = ortho.shape[1]

    def whole(shape):
        return pl.BlockSpec(shape, lambda i: (0, 0))

    return pl.pallas_call(
        functools.partial(weight_kernel, step_scale),
        grid=(height // rows,),
        out_shape=jax.ShapeDtypeStruct(weight.shape, weight.dtype),
        in_specs=[
            pl.BlockSpec((rows, width), lambda i: (i, 0)),
            pl.BlockSpec((rows, rank), lambda i: (i, 0)),
            whole((width, rank)),
            whole((1, rank)),
        ],
        out_specs=pl.BlockSpec((rows, width), lambda i: (i, 0)),
        scratch_shapes=[pltpu.VMEM((width, rank), jnp.bfloat16)] * 2,
        compiler_params=pltpu.CompilerParams(vmem_limit_bytes=60 * 1024 * 1024),
        cost_estimate=pl.CostEstimate(
            flops=6 * height * width * rank, bytes_accessed=4 * height * width, transcendentals=0
        ),
        name="weight_update",
    )(weight, ortho, projected, norm)


def meet(*values):
    return lax.optimization_barrier(values)


def low_bit(number):
    return number & -number


def children(number, size):
    bit = (low_bit(number) if number else size) // 2
    while bit:
        yield number | bit
        bit //= 2


def swap(block, axis, size, hop):
    return lax.ppermute(block, axis, [(i, i ^ hop) for i in range(size)])


def exchange_gather(block, axis, size, use=None, wire=None, meanwhile=None):
    blocks, coming = {}, {0: block if wire is None else pack(block, wire)}
    order = sorted(range(size), key=lambda m: (bin(m).count("1"), -m))
    if size == 8:
        order = [0, 2, 1, 4, 3, 6, 5, 7]
    state = None

    def receive(m):
        for child in children(m, size):
            coming[child] = swap(coming[m], axis, size, low_bit(child))
        blocks[m] = coming[m] if wire is None else unpack(coming[m], wire)

    receive(order[0])
    if meanwhile is not None:
        coming[size // 2], *state = meet(coming[size // 2], *meanwhile())
    for place, m in enumerate(order):
        if use is None:
            if place:
                receive(m)
            continue
        if place == 1:
            coming[m], *state = meet(coming[m], *state)
            receive(m)
        if 0 < place < size - 1:
            later = order[place + 1]
            coming[later], *state = meet(coming[later], *state)
            receive(later)
        state = use(m, blocks[m], state)
    return blocks, state


def scatter_order(size):
    return sorted(range(1, size), key=lambda m: (low_bit(m), -m))


def paced_scatter(make, operand, axis, size, bounds, beside):
    leaves = sorted(range(1, size, 2), reverse=True)
    inner = sorted(range(2, size, 2), key=lambda m: (low_bit(m), -m))
    if size == 8:
        inner = [6, 4, 2]
    parts, arrived, last = {}, {}, None

    def level(m):
        return low_bit(m).bit_length() - 1

    def send(m):
        wire = scale_of(bounds.levels[level(m)])
        arrived[m] = swap(pack(parts[m], wire), axis, size, low_bit(m))

    def value(m):
        return unpack(arrived[m], scale_of(bounds.partners[level(m)]))

    for place, m in enumerate(leaves + inner + [0]):
        if last is not None:
            *operand, parts[last] = meet(*operand, parts[last])
            if last % 2:
                send(last)
        if 0 <= place - 3 < len(leaves):
            behind = leaves[place - 3]
            *operand, arrived[behind] = meet(*operand, arrived[behind])
        operand = beside(place, operand)
        parts[m] = make(m, operand)
        last = m
    *operand, parts[last] = meet(*operand, parts[last])
    for m in sorted(range(0, size, 2), key=lambda m: (low_bit(m) if m else size, -m)):
        parts[m] = parts[m] + value(m | 1)
        for child in children(m, size):
            if child != m | 1:
                parts[m] = parts[m] + value(child)
        if m:
            send(m)
    return parts[0], operand


def matrix_sum(value, axis, size, index, beside):
    value = value + swap(value, axis, size, 1)
    mine = lax.dynamic_index_in_dim(
        value.reshape((2, -1) + value.shape[1:]), index % 2, 0, keepdims=False
    )
    hop = 2
    while hop < size:
        coming = swap(mine, axis, size, hop)
        if hop == 2:
            coming, *held = meet(coming, *beside.values())
            beside = dict(zip(beside, held))
        mine = mine + coming
        hop *= 2
    other = swap(mine, axis, size, 1)
    even = index % 2 == 0
    whole = jnp.concatenate([jnp.where(even, mine, other), jnp.where(even, other, mine)])
    return whole, beside


class HalvingSum:
    def __init__(self, blocks, axis, size, index):
        self.blocks, self.axis, self.size, self.index = blocks, axis, size, index
        self.hop = 1

    def send(self):
        bit = (self.index // self.hop) % 2
        pairs = self.blocks.reshape((-1, 2) + self.blocks.shape[1:])
        self.mine = lax.dynamic_index_in_dim(pairs, bit, 1, keepdims=False)
        other = lax.dynamic_index_in_dim(pairs, 1 - bit, 1, keepdims=False)
        self.coming = swap(other, self.axis, self.size, self.hop)

    def receive(self, operand):
        *operand, self.coming = meet(*operand, self.coming)
        self.blocks = self.mine + self.coming
        self.hop *= 2
        if self.hop < self.size:
            self.send()
        return operand


def pack(block, wire):
    return (block * wire).astype(jnp.float16)


def unpack(block, wire):
    return block.astype(jnp.float32) / wire


class Bounds:
    def __init__(self, own, extra, axis, size):
        self.levels, self.partners = [jnp.broadcast_to(own, (1, 128))], []
        self.extra = jnp.broadcast_to(extra, (1, 128))
        self.axis, self.size = axis, size

    def send(self):
        message = jnp.concatenate([self.levels[-1], self.extra])
        self.coming = swap(message, self.axis, self.size, 1 << len(self.partners))

    def receive(self, operand):
        *operand, self.coming = meet(*operand, self.coming)
        self.partners.append(self.coming[:1])
        self.levels.append(self.levels[-1] + self.coming[:1])
        self.extra = jnp.maximum(self.extra, self.coming[1:])
        if 1 << len(self.partners) < self.size:
            self.send()
        return operand


def scale_of(bound):
    return 32768.0 / jnp.maximum(bound[0, 0], 1e-30)


def magnitude(value):
    return jnp.max(jnp.abs(value.astype(jnp.float32)))


def assemble(blocks, index):
    size = len(blocks)
    first = blocks[0]
    whole = jnp.zeros((size,) + first.shape, first.dtype)
    for m in range(size):
        whole = lax.dynamic_update_index_in_dim(whole, blocks[m], index ^ m, 0)
    return whole.reshape((size * first.shape[0],) + first.shape[1:])


def make_body(rows_n, cols_n, step_scale):
    def body(weight, momentum, right_factor, output_grads, activations):
        row = lax.axis_index("row")
        col = lax.axis_index("col")
        tile_rows, tile_cols = momentum.shape
        rank = right_factor.shape[1]
        share = tile_rows // cols_n
        momentum_blocks = momentum.reshape(cols_n, share, tile_cols)

        tokens = output_grads.shape[0]
        grads_blocks = output_grads.reshape(tokens, cols_n, share).transpose(1, 0, 2)
        grads_own = lax.all_to_all(grads_blocks, "col", split_axis=0, concat_axis=0, tiled=True)
        grads_own = grads_own.reshape(-1, share)
        factor_blocks, (largest,) = exchange_gather(
            right_factor, "row", rows_n, meanwhile=lambda: [magnitude(momentum)]
        )
        factor_whole = assemble(factor_blocks, row)

        token_part = dot(activations.astype(jnp.float32), factor_whole, (1, 0), HIGH)
        factor_whole, token_part = meet(factor_whole, token_part)
        bounds = Bounds(
            tile_cols * largest * magnitude(factor_whole), magnitude(output_grads), "col", cols_n
        )
        depth = min(512, tile_cols)
        factor = [v.reshape(-1, depth, rank) for v in split_outside(factor_whole)]

        def make(m, operand):
            return part_product(jnp.stack([col ^ m]), momentum_blocks, *operand)

        token_parts = HalvingSum(token_part.reshape(cols_n, -1, rank), "col", cols_n, col)
        gathers = {}

        def beside(place, operand):
            if place == 0:
                token_parts.send()
                bounds.send()
            elif token_parts.hop < cols_n:
                operand = token_parts.receive(operand)
                operand = bounds.receive(operand)
                if place == 2:
                    *operand, gathers["own"] = meet(*operand, grads_own)
                if token_parts.hop == cols_n:
                    gathers["tokens"] = lax.all_gather(
                        token_parts.blocks[0], ("row", "col"), axis=0, tiled=True
                    )
            return operand

        left_own, factor = paced_scatter(make, factor, "col", cols_n, bounds, beside)
        token_sums = gathers["tokens"]
        left_own = left_own + dot(gathers["own"].astype(jnp.float32), token_sums, (0, 0), HIGH)
        wire = scale_of(
            bounds.levels[-1] + (tokens * cols_n) * bounds.extra * magnitude(token_sums)
        )
        left_own, acts_whole = meet(left_own, activations)
        acts_whole = lax.all_gather(acts_whole, "row", axis=0, tiled=True)

        chunk = min(512, tile_cols)

        seen = []

        def use(m, block, state):
            if len(seen) == 2:
                *state, gathers["acts"], grads_first = meet(
                    *state, acts_whole, output_grads[:, : 3 * tile_rows // 8]
                )
                gathers["grads"] = lax.all_gather(grads_first, "col", axis=0, tiled=True)
            seen.append(m)
            return step_product(
                jnp.stack([col ^ m]), block, momentum_blocks, grads_blocks, state, chunk
            )

        left_blocks, state = exchange_gather(left_own, "col", cols_n, use, wire)
        acts_whole = gathers["acts"]
        product, small = state
        piece = tile_cols // rows_n

        def product_piece(m):
            if piece == chunk:
                return lax.dynamic_index_in_dim(product, row ^ m, 0, keepdims=False)
            whole = product.transpose(1, 0, 2).reshape(rank, tile_cols)
            return lax.dynamic_slice_in_dim(whole, (row ^ m) * piece, piece, 1)

        pieces = {m: product_piece(m) for m in range(rows_n)}
        pieces = {m: pieces[m] + swap(pieces[m | 1], "row", rows_n, 1) for m in range(0, rows_n, 2)}
        small, pieces = matrix_sum(small, "row", rows_n, row, pieces)
        gram_matrix, token_left = small[:rank], small[rank:]
        token_left, gathers["grads"] = meet(token_left, gathers["grads"])
        token_left = lax.all_gather(token_left, "col", axis=0, tiled=True)
        for m in sorted(range(2, rows_n, 2), key=lambda m: (low_bit(m), -m)):
            hop = low_bit(m)
            pieces[m ^ hop] = pieces[m ^ hop] + swap(pieces[m], "row", rows_n, hop)
        grads_last, gram_matrix = meet(output_grads[:, 3 * tile_rows // 8 :], gram_matrix)
        grads_last = lax.all_gather(grads_last, "col", axis=0, tiled=True)

        inverse = inverse_factor(gram_matrix)
        product_own = late_product(jnp.stack([row]), acts_whole, token_left, pieces[0])
        projected_own = dot(product_own, inverse, (0, 1), FULL)

        squares = jnp.sum(projected_own * projected_own, axis=0, keepdims=True)
        hops = [("col", cols_n, 1 << i) for i in range(cols_n.bit_length() - 1)]
        hops += [("row", rows_n, 1 << i) for i in range(rows_n.bit_length() - 1)]
        near = cols_n.bit_length()
        def meanwhile():
            sums, operand, blocks = squares, inverse, {}
            for m in range(cols_n):
                coming = swap(sums, *hops[m]) if m < near else None
                blocks[m] = dot(left_blocks[m], operand, (1, 1), HIGH)
                if coming is not None:
                    coming, operand, blocks[m] = meet(coming, operand, blocks[m])
                    sums = sums + coming
            return [assemble(blocks, col), sums]

        projected_blocks, (ortho_left, squares) = exchange_gather(
            projected_own, "row", rows_n, meanwhile=meanwhile
        )
        projected = assemble(projected_blocks, row)
        for hop in hops[near:]:
            squares = squares + swap(squares, *hop)
        column_norm = jnp.sqrt(squares + NORM_EPS)
        new_factor = projected_own / column_norm

        new_weight = weight_update(
            weight, ortho_left, projected, column_norm, step_scale
        )
        new_weight, grads_last = meet(new_weight, grads_last)
        new_momentum = momentum_update(
            momentum, (gathers["grads"], grads_last), acts_whole, ortho_left, projected
        )
        return (new_weight, new_momentum, new_factor)

    return body


def solution(mesh):
    rows_n, cols_n = mesh.shape["row"], mesh.shape["col"]
    in_specs = (
        P("row", "col"),
        P("row", "col"),
        P(("col", "row"), None),
        P("col", "row"),
        P("row", "col"),
    )
    out_specs = (P("row", "col"), P("row", "col"), P(("col", "row"), None))

    def step(weight, momentum, right_factor, output_grads, activations):
        step_scale = LEARN_RATE * math.sqrt(max(weight.shape))
        return jax.shard_map(
            make_body(rows_n, cols_n, step_scale),
            mesh=mesh,
            in_specs=in_specs,
            out_specs=out_specs,
            check_vma=False,
        )(weight, momentum, right_factor, output_grads, activations)

    return step
```

```python
import functools
import math

import jax
import jax.numpy as jnp
from jax import lax
from jax.experimental import pallas as pl
from jax.experimental.pallas import tpu as pltpu
from jax.sharding import PartitionSpec as P

FULL = lax.Precision.HIGHEST
HIGH = lax.Precision.HIGH
MOMENTUM_DECAY = 0.95
LEARN_RATE = 0.002
NORM_EPS = 1e-06
SIDE = 128
PANEL = 8


def dot(first, second, dims, precision=None):
    return lax.dot_general(
        first,
        second,
        (((dims[0],), (dims[1],)), ((), ())),
        precision=precision,
        preferred_element_type=jnp.float32,
    )


def full_dot(first, second, dims):
    return lax.dot_general(first, second, (((dims[0],), (dims[1],)), ((), ())), precision=FULL, preferred_element_type=jnp.float32)


def factor_kernel(gram_ref, inverse_ref, work, pair):
    size = gram_ref.shape[0]
    count = size // SIDE
    work[...] = gram_ref[...]
    inverse_ref[...] = jnp.zeros_like(inverse_ref)
    lane = lax.broadcasted_iota(jnp.int32, (PANEL, 2 * SIDE), 1)
    line = lax.broadcasted_iota(jnp.int32, (PANEL, 1), 0)
    eye = (lax.broadcasted_iota(jnp.int32, (SIDE, SIDE), 0) == lax.broadcasted_iota(jnp.int32, (SIDE, SIDE), 1)).astype(jnp.float32)

    def eliminate(step, carry):
        base = pl.multiple_of(step * PANEL, PANEL)
        rows = pair[pl.ds(base, PANEL), :]
        columns = [
            jnp.sum(jnp.where(lane == base + j, rows, 0.0), axis=1, keepdims=True)
            for j in range(PANEL)
        ]
        for j in range(PANEL):
            pivot = columns[j][j : j + 1, :]
            root = lax.rsqrt(pivot)
            root = root * (1.5 - 0.5 * pivot * root * root)
            below = jnp.where(line > j, columns[j] * root, 0.0)
            scaled = rows[j : j + 1, :] * root
            rows = jnp.where(line == j, scaled, rows - below * scaled)
            for i in range(j + 1, PANEL):
                columns[i] = columns[i] - below * (columns[i][j : j + 1, :] * root)
        pair[pl.ds(base, PANEL), :] = rows
        later = jnp.where(lane >= base + PANEL, rows, 0.0)[:, :SIDE]
        pair[...] = pair[...] - full_dot(later, rows, (0, 0))
        return carry

    for k in range(count):
        here = slice(k * SIDE, (k + 1) * SIDE)
        pair[:, :SIDE] = work[here, here]
        pair[:, SIDE:] = eye
        lax.fori_loop(0, SIDE // PANEL, eliminate, 0)
        diagonal = pair[:, SIDE:]
        inverse_ref[here, here] = diagonal
        if k:
            inverse_ref[here, : k * SIDE] = full_dot(diagonal, inverse_ref[here, : k * SIDE], (1, 0))
        if k + 1 < count:
            after = slice((k + 1) * SIDE, size)
            strip = full_dot(work[after, here], diagonal, (1, 1))
            work[after, after] = work[after, after] - full_dot(strip, strip, (1, 1))
            done = (k + 1) * SIDE
            inverse_ref[after, :done] = inverse_ref[after, :done] - full_dot(strip, inverse_ref[here, :done], (1, 0))


def inverse_factor(gram_matrix):
    size = gram_matrix.shape[0]
    return pl.pallas_call(
        factor_kernel,
        out_shape=jax.ShapeDtypeStruct(gram_matrix.shape, jnp.float32),
        in_specs=[pl.BlockSpec(memory_space=pltpu.VMEM)],
        out_specs=pl.BlockSpec(memory_space=pltpu.VMEM),
        scratch_shapes=[
            pltpu.VMEM((size, size), jnp.float32),
            pltpu.VMEM((SIDE, 2 * SIDE), jnp.float32),
        ],
        name="inverse_factor",
    )(gram_matrix)


def split(value):
    high = value.astype(jnp.bfloat16)
    low = (value - high.astype(jnp.float32)).astype(jnp.bfloat16)
    return high, low


def split_outside(value):
    high = lax.reduce_precision(value, 8, 7)
    return high.astype(jnp.bfloat16), (value - high).astype(jnp.bfloat16)


def part_kernel(place, old, high, low, out):
    first, rest = split(old[0])
    total = dot(first, high[0], (1, 0)) + dot(rest, high[0], (1, 0)) + dot(first, low[0], (1, 0))

    @pl.when(pl.program_id(0) == 0)
    def _():
        out[...] = total

    @pl.when(pl.program_id(0) > 0)
    def _():
        out[...] = out[...] + total


def part_product(place, blocks, high, low):
    _, height, width = blocks.shape
    count, depth, rank = high.shape
    return pl.pallas_call(
        part_kernel,
        grid_spec=pltpu.PrefetchScalarGridSpec(
            num_scalar_prefetch=1,
            grid=(count,),
            in_specs=[
                pl.BlockSpec((1, height, depth), lambda j, place: (place[0], 0, j)),
                pl.BlockSpec((1, depth, rank), lambda j, place: (j, 0, 0)),
                pl.BlockSpec((1, depth, rank), lambda j, place: (j, 0, 0)),
            ],
            out_specs=pl.BlockSpec((height, rank), lambda j, place: (0, 0)),
        ),
        out_shape=jax.ShapeDtypeStruct((height, rank), jnp.float32),
        compiler_params=pltpu.CompilerParams(vmem_limit_bytes=32 * 1024 * 1024),
        cost_estimate=pl.CostEstimate(
            flops=6 * height * width * rank, bytes_accessed=4 * height * width, transcendentals=0
        ),
        name="part_product",
    )(place, blocks, high, low)


def step_kernel(started, place, block, old, grads, *refs):
    before, (product, small, high_t, low_t) = refs[:-4], refs[-4:]
    rank = block.shape[1]

    @pl.when(pl.program_id(0) == 0)
    def _():
        high, low = split(block[...])
        high_t[...] = high.T
        low_t[...] = low.T
        new_gram = (
            dot(high_t[...], high, (1, 0))
            + dot(high_t[...], low, (1, 0))
            + dot(low_t[...], high, (1, 0))
            + dot(low_t[...], low, (1, 0))
        )
        new_tokens = dot(grads[0], high, (1, 0)) + dot(grads[0], low, (1, 0))
        small[:rank] = before[1][:rank] + new_gram if started else new_gram
        small[rank:] = before[1][rank:] + new_tokens if started else new_tokens

    first, rest = split(old[0])
    total = (
        dot(high_t[...], first, (1, 0))
        + dot(low_t[...], first, (1, 0))
        + dot(high_t[...], rest, (1, 0))
    )
    product[0] = before[0][0] + total if started else total


def step_product(place, block, blocks, grads, before, chunk):
    _, height, width = blocks.shape
    rank = block.shape[1]
    tokens = grads.shape[1]
    started = before is not None
    shapes = [(width // chunk, rank, chunk), (rank + tokens, rank)]
    specs = [
        pl.BlockSpec((1, rank, chunk), lambda j, place: (j, 0, 0)),
        pl.BlockSpec((rank + tokens, rank), lambda j, place: (0, 0)),
    ]
    return pl.pallas_call(
        functools.partial(step_kernel, started),
        grid_spec=pltpu.PrefetchScalarGridSpec(
            num_scalar_prefetch=1,
            grid=(width // chunk,),
            in_specs=[
                pl.BlockSpec((height, rank), lambda j, place: (0, 0)),
                pl.BlockSpec((1, height, chunk), lambda j, place: (place[0], 0, j)),
                pl.BlockSpec((1, tokens, height), lambda j, place: (place[0], 0, 0)),
            ]
            + (specs if started else []),
            out_specs=specs,
            scratch_shapes=[
                pltpu.VMEM((rank, height), jnp.bfloat16),
                pltpu.VMEM((rank, height), jnp.bfloat16),
            ],
        ),
        out_shape=[jax.ShapeDtypeStruct(shape, jnp.float32) for shape in shapes],
        compiler_params=pltpu.CompilerParams(vmem_limit_bytes=40 * 1024 * 1024),
        cost_estimate=pl.CostEstimate(
            flops=6 * height * width * rank, bytes_accessed=4 * height * width, transcendentals=0
        ),
        input_output_aliases={4: 0, 5: 1} if started else {},
        name="step_product",
    )(place, block, blocks, grads, *(before or ()))


def late_kernel(place, acts, tokens, base, out):
    high, low = split(tokens[...])
    out[...] = base[...] + dot(high, acts[...], (0, 0)) + dot(low, acts[...], (0, 0))


def late_product(place, acts, tokens, base):
    count, rank = tokens.shape
    width = base.shape[1]
    if width % 128:
        block = lax.dynamic_slice_in_dim(acts, place[0] * width, width, 1)
        return base + dot(tokens, block.astype(jnp.float32), (0, 0), HIGH)
    return pl.pallas_call(
        late_kernel,
        grid_spec=pltpu.PrefetchScalarGridSpec(
            num_scalar_prefetch=1,
            grid=(1,),
            in_specs=[
                pl.BlockSpec((count, width), lambda i, place: (0, place[0])),
                pl.BlockSpec((count, rank), lambda i, place: (0, 0)),
                pl.BlockSpec((rank, width), lambda i, place: (0, 0)),
            ],
            out_specs=pl.BlockSpec((rank, width), lambda i, place: (0, 0)),
        ),
        out_shape=jax.ShapeDtypeStruct((rank, width), jnp.float32),
        compiler_params=pltpu.CompilerParams(vmem_limit_bytes=40 * 1024 * 1024),
        cost_estimate=pl.CostEstimate(
            flops=4 * count * rank * width, bytes_accessed=6 * count * width, transcendentals=0
        ),
        name="late_product",
    )(place, acts, tokens, base)


def momentum_kernel(old, grads_a, grads_b, acts, ortho, projected, new):
    width = new.shape[1]
    step = min(512, width)
    turned = ((MOMENTUM_DECAY - 1.0) * ortho[...]).astype(jnp.bfloat16)

    def fill(grads):
        for start in range(0, width, step):
            here = slice(start, start + step)
            total = dot(turned, projected[here, :].astype(jnp.bfloat16), (1, 1))
            total += dot(grads[...], acts[:, here], (0, 0))
            new[:, here] = old[:, here] + total

    early = pl.program_id(0) < pl.num_programs(0) // 2
    pl.when(early)(lambda: fill(grads_a))
    pl.when(jnp.logical_not(early))(lambda: fill(grads_b))


def momentum_update(momentum, grads, acts, ortho, projected):
    height, width = momentum.shape
    rows = min(512, height // 2)
    count = height // rows
    first = count // 2
    rank = ortho.shape[1]
    tokens = acts.shape[0]

    def whole(shape):
        return pl.BlockSpec(shape, lambda i: (0, 0))

    return pl.pallas_call(
        momentum_kernel,
        grid=(count,),
        out_shape=jax.ShapeDtypeStruct(momentum.shape, jnp.float32),
        in_specs=[
            pl.BlockSpec((rows, width), lambda i: (i, 0)),
            pl.BlockSpec((tokens, rows), lambda i: (0, jnp.minimum(i, first - 1))),
            pl.BlockSpec((tokens, rows), lambda i: (0, jnp.maximum(i - first, 0))),
            whole((tokens, width)),
            pl.BlockSpec((rows, rank), lambda i: (i, 0)),
            whole((width, rank)),
        ],
        out_specs=pl.BlockSpec((rows, width), lambda i: (i, 0)),
        compiler_params=pltpu.CompilerParams(vmem_limit_bytes=60 * 1024 * 1024),
        cost_estimate=pl.CostEstimate(
            flops=2 * height * width * (tokens + rank),
            bytes_accessed=8 * height * width,
            transcendentals=0,
        ),
        name="momentum_update",
    )(momentum, *grads, acts, ortho, projected)


def weight_kernel(step_scale, old, ortho, projected, norm, new, factor_high, factor_low):
    @pl.when(pl.program_id(0) == 0)
    def _():
        factor_high[...], factor_low[...] = split(projected[...] / norm[...])

    width = new.shape[1]
    step = min(512, width)
    first, rest = split(ortho[...])
    for start in range(0, width, step):
        here = slice(start, start + step)
        total = dot(first, factor_high[here, :], (1, 1))
        total += dot(rest, factor_high[here, :], (1, 1))
        total += dot(first, factor_low[here, :], (1, 1))
        new[:, here] = (old[:, here].astype(jnp.float32) - step_scale * total).astype(new.dtype)


def weight_update(weight, ortho, projected, norm, step_scale):
    height, width = weight.shape
    rows = min(512, height)
    rank = ortho.shape[1]

    def whole(shape):
        return pl.BlockSpec(shape, lambda i: (0, 0))

    return pl.pallas_call(
        functools.partial(weight_kernel, step_scale),
        grid=(height // rows,),
        out_shape=jax.ShapeDtypeStruct(weight.shape, weight.dtype),
        in_specs=[
            pl.BlockSpec((rows, width), lambda i: (i, 0)),
            pl.BlockSpec((rows, rank), lambda i: (i, 0)),
            whole((width, rank)),
            whole((1, rank)),
        ],
        out_specs=pl.BlockSpec((rows, width), lambda i: (i, 0)),
        scratch_shapes=[pltpu.VMEM((width, rank), jnp.bfloat16)] * 2,
        compiler_params=pltpu.CompilerParams(vmem_limit_bytes=60 * 1024 * 1024),
        cost_estimate=pl.CostEstimate(
            flops=6 * height * width * rank, bytes_accessed=4 * height * width, transcendentals=0
        ),
        name="weight_update",
    )(weight, ortho, projected, norm)


def meet(*values):
    return lax.optimization_barrier(values)


def low_bit(number):
    return number & -number


def children(number, size):
    bit = (low_bit(number) if number else size) // 2
    while bit:
        yield number | bit
        bit //= 2


def swap(block, axis, size, hop):
    return lax.ppermute(block, axis, [(i, i ^ hop) for i in range(size)])


def exchange_gather(block, axis, size, use=None, wire=None, meanwhile=None):
    blocks, coming = {}, {0: block if wire is None else pack(block, wire)}
    order = sorted(range(size), key=lambda m: (bin(m).count("1"), -m))
    if size == 8:
        order = [0, 2, 1, 4, 3, 6, 5, 7]
    state = None

    def receive(m):
        for child in children(m, size):
            coming[child] = swap(coming[m], axis, size, low_bit(child))
        blocks[m] = coming[m] if wire is None else unpack(coming[m], wire)

    receive(order[0])
    if meanwhile is not None:
        coming[size // 2], *state = meet(coming[size // 2], *meanwhile())
    for place, m in enumerate(order):
        if use is None:
            if place:
                receive(m)
            continue
        if place == 1:
            coming[m], *state = meet(coming[m], *state)
            receive(m)
        if 0 < place < size - 1:
            later = order[place + 1]
            coming[later], *state = meet(coming[later], *state)
            receive(later)
        state = use(m, blocks[m], state)
    return blocks, state


def scatter_order(size):
    return sorted(range(1, size), key=lambda m: (low_bit(m), -m))


def paced_scatter(make, operand, axis, size, bounds, beside):
    leaves = sorted(range(1, size, 2), reverse=True)
    inner = sorted(range(2, size, 2), key=lambda m: (low_bit(m), -m))
    if size == 8:
        inner = [6, 4, 2]
    parts, arrived, last = {}, {}, None

    def level(m):
        return low_bit(m).bit_length() - 1

    def send(m):
        wire = scale_of(bounds.levels[level(m)])
        arrived[m] = swap(pack(parts[m], wire), axis, size, low_bit(m))

    def value(m):
        return unpack(arrived[m], scale_of(bounds.partners[level(m)]))

    for place, m in enumerate(leaves + inner + [0]):
        if last is not None:
            *operand, parts[last] = meet(*operand, parts[last])
            if last % 2:
                send(last)
        if 0 <= place - 3 < len(leaves):
            behind = leaves[place - 3]
            *operand, arrived[behind] = meet(*operand, arrived[behind])
        operand = beside(place, operand)
        parts[m] = make(m, operand)
        last = m
    *operand, parts[last] = meet(*operand, parts[last])
    for m in sorted(range(0, size, 2), key=lambda m: (low_bit(m) if m else size, -m)):
        parts[m] = parts[m] + value(m | 1)
        for child in children(m, size):
            if child != m | 1:
                parts[m] = parts[m] + value(child)
        if m:
            send(m)
    return parts[0], operand


def matrix_sum(value, axis, size, index, beside):
    value = value + swap(value, axis, size, 1)
    mine = lax.dynamic_index_in_dim(
        value.reshape((2, -1) + value.shape[1:]), index % 2, 0, keepdims=False
    )
    hop = 2
    while hop < size:
        coming = swap(mine, axis, size, hop)
        if hop == 2:
            coming, *held = meet(coming, *beside.values())
            beside = dict(zip(beside, held))
        mine = mine + coming
        hop *= 2
    other = swap(mine, axis, size, 1)
    even = index % 2 == 0
    whole = jnp.concatenate([jnp.where(even, mine, other), jnp.where(even, other, mine)])
    return whole, beside


class HalvingSum:
    def __init__(self, blocks, axis, size, index):
        self.blocks, self.axis, self.size, self.index = blocks, axis, size, index
        self.hop = 1

    def send(self):
        bit = (self.index // self.hop) % 2
        pairs = self.blocks.reshape((-1, 2) + self.blocks.shape[1:])
        self.mine = lax.dynamic_index_in_dim(pairs, bit, 1, keepdims=False)
        other = lax.dynamic_index_in_dim(pairs, 1 - bit, 1, keepdims=False)
        self.coming = swap(other, self.axis, self.size, self.hop)

    def receive(self, operand):
        *operand, self.coming = meet(*operand, self.coming)
        self.blocks = self.mine + self.coming
        self.hop *= 2
        if self.hop < self.size:
            self.send()
        return operand


def pack(block, wire):
    return (block * wire).astype(jnp.float16)


def unpack(block, wire):
    return block.astype(jnp.float32) / wire


class Bounds:
    def __init__(self, own, extra, axis, size):
        self.levels, self.partners = [jnp.broadcast_to(own, (1, 128))], []
        self.extra = jnp.broadcast_to(extra, (1, 128))
        self.axis, self.size = axis, size

    def send(self):
        message = jnp.concatenate([self.levels[-1], self.extra])
        self.coming = swap(message, self.axis, self.size, 1 << len(self.partners))

    def receive(self, operand):
        *operand, self.coming = meet(*operand, self.coming)
        self.partners.append(self.coming[:1])
        self.levels.append(self.levels[-1] + self.coming[:1])
        self.extra = jnp.maximum(self.extra, self.coming[1:])
        if 1 << len(self.partners) < self.size:
            self.send()
        return operand


def scale_of(bound):
    return 32768.0 / jnp.maximum(bound[0, 0], 1e-30)


def magnitude(value):
    return jnp.max(jnp.abs(value.astype(jnp.float32)))


def assemble(blocks, index):
    size = len(blocks)
    first = blocks[0]
    whole = jnp.zeros((size,) + first.shape, first.dtype)
    for m in range(size):
        whole = lax.dynamic_update_index_in_dim(whole, blocks[m], index ^ m, 0)
    return whole.reshape((size * first.shape[0],) + first.shape[1:])


def make_body(rows_n, cols_n, step_scale):
    def body(weight, momentum, right_factor, output_grads, activations):
        row = lax.axis_index("row")
        col = lax.axis_index("col")
        tile_rows, tile_cols = momentum.shape
        rank = right_factor.shape[1]
        share = tile_rows // cols_n
        momentum_blocks = momentum.reshape(cols_n, share, tile_cols)

        tokens = output_grads.shape[0]
        grads_blocks = output_grads.reshape(tokens, cols_n, share).transpose(1, 0, 2)
        grads_own = lax.all_to_all(grads_blocks, "col", split_axis=0, concat_axis=0, tiled=True)
        grads_own = grads_own.reshape(-1, share)
        factor_blocks, (largest,) = exchange_gather(
            right_factor, "row", rows_n, meanwhile=lambda: [magnitude(momentum)]
        )
        largest, grads_own, acts_own, *met = meet(
            largest, grads_own, activations, *[factor_blocks[m] for m in range(rows_n)]
        )
        acts_whole = lax.all_gather(acts_own, "row", axis=0, tiled=True)
        factor_whole = assemble(dict(enumerate(met)), row)

        token_part = dot(activations.astype(jnp.float32), factor_whole, (1, 0), HIGH)
        factor_whole, token_part = meet(factor_whole, token_part)
        bounds = Bounds(
            tile_cols * largest * magnitude(factor_whole), magnitude(output_grads), "col", cols_n
        )
        depth = min(512, tile_cols)
        factor = [v.reshape(-1, depth, rank) for v in split_outside(factor_whole)]

        def make(m, operand):
            return part_product(jnp.stack([col ^ m]), momentum_blocks, *operand)

        token_parts = HalvingSum(token_part.reshape(cols_n, -1, rank), "col", cols_n, col)
        gathers = {}

        def beside(place, operand):
            if place == 0:
                token_parts.send()
                bounds.send()
            elif token_parts.hop < cols_n:
                operand = token_parts.receive(operand)
                operand = bounds.receive(operand)
                if token_parts.hop == cols_n:
                    share_sum, gathers["acts"] = meet(token_parts.blocks[0], acts_whole)
                    gathers["tokens"] = lax.all_gather(
                        share_sum, ("row", "col"), axis=0, tiled=True
                    )
            return operand

        left_own, factor = paced_scatter(make, factor, "col", cols_n, bounds, beside)
        token_sums = gathers["tokens"]
        left_own = left_own + dot(grads_own.astype(jnp.float32), token_sums, (0, 0), HIGH)
        wire = scale_of(
            bounds.levels[-1] + (tokens * cols_n) * bounds.extra * magnitude(token_sums)
        )
        left_own, grads_first = meet(left_own, output_grads[:, : tile_rows // 2])
        grads_first = lax.all_gather(grads_first, "col", axis=0, tiled=True)

        chunk = min(512, tile_cols)

        def use(m, block, state):
            return step_product(
                jnp.stack([col ^ m]), block, momentum_blocks, grads_blocks, state, chunk
            )

        left_blocks, state = exchange_gather(left_own, "col", cols_n, use, wire)
        acts_whole = gathers["acts"]
        product, small = state
        piece = tile_cols // rows_n

        def product_piece(m):
            if piece == chunk:
                return lax.dynamic_index_in_dim(product, row ^ m, 0, keepdims=False)
            whole = product.transpose(1, 0, 2).reshape(rank, tile_cols)
            return lax.dynamic_slice_in_dim(whole, (row ^ m) * piece, piece, 1)

        pieces = {m: product_piece(m) for m in range(rows_n)}
        pieces = {m: pieces[m] + swap(pieces[m | 1], "row", rows_n, 1) for m in range(0, rows_n, 2)}
        small, pieces = matrix_sum(small, "row", rows_n, row, pieces)
        gram_matrix, token_left = small[:rank], small[rank:]
        token_left, grads_first = meet(token_left, grads_first)
        token_left = lax.all_gather(token_left, "col", axis=0, tiled=True)
        for m in sorted(range(2, rows_n, 2), key=lambda m: (low_bit(m), -m)):
            hop = low_bit(m)
            pieces[m ^ hop] = pieces[m ^ hop] + swap(pieces[m], "row", rows_n, hop)
        grads_last, gram_matrix = meet(output_grads[:, tile_rows // 2 :], gram_matrix)
        grads_last = lax.all_gather(grads_last, "col", axis=0, tiled=True)

        inverse = inverse_factor(gram_matrix)
        product_own = late_product(jnp.stack([row]), acts_whole, token_left, pieces[0])
        projected_own = dot(product_own, inverse, (0, 1), FULL)

        squares = jnp.sum(projected_own * projected_own, axis=0, keepdims=True)
        hops = [("col", cols_n, 1 << i) for i in range(cols_n.bit_length() - 1)]
        hops += [("row", rows_n, 1 << i) for i in range(rows_n.bit_length() - 1)]
        near = cols_n.bit_length()
        def meanwhile():
            sums, operand, blocks = squares, inverse, {}
            for m in range(cols_n):
                coming = swap(sums, *hops[m]) if m < near else None
                blocks[m] = dot(left_blocks[m], operand, (1, 1), HIGH)
                if coming is not None:
                    coming, operand, blocks[m] = meet(coming, operand, blocks[m])
                    sums = sums + coming
            return [assemble(blocks, col), sums]

        projected_blocks, (ortho_left, squares) = exchange_gather(
            projected_own, "row", rows_n, meanwhile=meanwhile
        )
        projected = assemble(projected_blocks, row)
        for hop in hops[near:]:
            squares = squares + swap(squares, *hop)
        column_norm = jnp.sqrt(squares + NORM_EPS)
        new_factor = projected_own / column_norm

        new_weight = weight_update(
            weight, ortho_left, projected, column_norm, step_scale
        )
        new_weight, grads_last = meet(new_weight, grads_last)
        new_momentum = momentum_update(
            momentum, (grads_first, grads_last), acts_whole, ortho_left, projected
        )
        return (new_weight, new_momentum, new_factor)

    return body


def solution(mesh):
    rows_n, cols_n = mesh.shape["row"], mesh.shape["col"]
    in_specs = (
        P("row", "col"),
        P("row", "col"),
        P(("col", "row"), None),
        P("col", "row"),
        P("row", "col"),
    )
    out_specs = (P("row", "col"), P("row", "col"), P(("col", "row"), None))

    def step(weight, momentum, right_factor, output_grads, activations):
        step_scale = LEARN_RATE * math.sqrt(max(weight.shape))
        return jax.shard_map(
            make_body(rows_n, cols_n, step_scale),
            mesh=mesh,
            in_specs=in_specs,
            out_specs=out_specs,
            check_vma=False,
        )(weight, momentum, right_factor, output_grads, activations)

    return step
```
